128 devices in a mesh: area: 16 (over z, y), tie: 8 (over x, core).
Axes of the slice: x: 4, y: 4, z: 4, core: 2. Of those that a mesh axis runs over, the one named last changes fastest.
Arguments:
- ginv: bfloat16 [512, 1024, 1024], P(('area', 'tie'))
- rhs: float32 [524288, 128], P(('area', 'tie')), may hold values from -6 to 6
- bnd_row: int32 [512, 128], P(('area', 'tie')), may hold values from -1 to 1023, as said below
- bnd_var: int32 [512, 128], P(('area', 'tie')), may hold values from -1 to 8191, as said below
Outputs:
- states: float32 [524288, 128], P(('area', 'tie'))
- consensus: float32 [8192, 128], P(('area', 'tie'))
- dual_value: float32 [65536, 128], P(('area', 'tie'))
The draws below stay inside these ranges and needn't reach their ends.
Inputs may be any that keep to these rules, and one draw needn't show every extreme that they name: `bnd_row`: -1 marks an unused entry slot; the live rows of one area are distinct. `bnd_var`: -1 exactly where bnd_row is -1. Variable v is owned by the device holding rows v of the consensus output, block v // 64. The areas of one device hold at most 4 live entries owned by any one device; in every draw some owner holds exactly 4 from every device.
All inputs are finite; a program needn't handle non-finite values.
Results may differ from the reference program's by a relative error of at most 0.003.
Values sent between devices are 32-bit elements; how exact they have to be, the bound alone decides.
No kernel may reach another device: no remote copies, remote signals or barrier semaphores. Data moves between devices by JAX's collectives and lax.ppermute only.
A program may use at most 64 MiB of HBM per device.

```python
import jax
import jax.numpy as jnp
from jax import lax

STATE = 1024
BND = 128
SLOT = 4
VAR_DEV = 64
AREA_DEV = 4
SNAP = 128
ITERS = 4
AREAS = 512
VARS = 8192


def boundary_maps(key):
    device_total = AREAS // AREA_DEV
    entries = AREA_DEV * BND
    hottest = jax.random.randint(jax.random.fold_in(key, 11), (), 0, device_total)
    slot_counts = jax.random.randint(jax.random.fold_in(key, 12), (device_total, device_total), 1, SLOT + 1)
    owner_ids = jnp.arange(device_total, dtype=jnp.int32)
    slot_counts = jnp.where(owner_ids[None, :] == hottest, SLOT, slot_counts)
    slot_live = jnp.arange(SLOT)[None, None, :] < slot_counts[:, :, None]
    local_ids = jax.random.randint(jax.random.fold_in(key, 13), (device_total, device_total, SLOT), 0, VAR_DEV)
    var_slot = jnp.where(slot_live, owner_ids[None, :, None] * VAR_DEV + local_ids, -1)
    var_slot = var_slot.reshape(device_total, device_total * SLOT).astype(jnp.int32)
    perm_keys = jax.random.split(jax.random.fold_in(key, 14), device_total)
    placing = jax.vmap(lambda k: jax.random.permutation(k, entries))(perm_keys)[:, :device_total * SLOT]
    entry_var = jnp.full((device_total, entries), -1, jnp.int32)
    entry_var = entry_var.at[jnp.arange(device_total)[:, None], placing].set(var_slot)
    entry_var = entry_var.reshape(AREAS, BND)
    row_keys = jax.random.split(jax.random.fold_in(key, 15), AREAS)
    row_perm = jax.vmap(lambda k: jax.random.permutation(k, STATE))(row_keys)[:, :BND].astype(jnp.int32)
    entry_row = jnp.where(entry_var >= 0, row_perm, -1).astype(jnp.int32)
    return (entry_row, entry_var)


def draw_bnd_row(key, part):
    return boundary_maps(key)[0]


def draw_bnd_var(key, part):
    return boundary_maps(key)[1]


def draw_ginv(key, part):
    area_keys = jax.random.split(jax.random.fold_in(key, 21), AREAS)

    def one_block(block_key):
        diag_values = jax.random.uniform(jax.random.fold_in(block_key, 7), (STATE,), jnp.float32, 0.3, 0.85)
        noise = jax.random.normal(block_key, (STATE, STATE), jnp.float32)
        return (jnp.diag(diag_values) + 0.3 * noise / STATE ** 0.5).astype(jnp.bfloat16)
    return lax.map(one_block, area_keys)


def block_levels(key, dims, shards, smallest, top_value):
    def one(dim, blocks):
        heights = jax.random.uniform(jax.random.fold_in(jax.random.fold_in(key, 6), dim), (blocks,), jnp.float32, smallest / len(shards), top_value / len(shards))
        return jnp.repeat(jnp.exp(heights), dims[dim] // blocks).reshape((-1,) + (1,) * (len(dims) - dim - 1))

    loudness = one(*shards[0])
    for cut in shards[1:]:
        loudness = loudness * one(*cut)
    return loudness


def scatter_about(stream_key, dims, deviation, most, cuts=(), kind=jnp.bfloat16):
    values = jax.random.normal(stream_key, dims, jnp.float32) * deviation
    if len(cuts) > 0:
        values = block_levels(stream_key, dims, cuts, -0.22, 0.18) * values
    return jnp.clip(values, min=-most, max=most).astype(kind)


def setup_inputs(seed: int = 0) -> dict:
    seeds = jax.random.split(jax.random.key(seed), 5)
    return {
        "ginv": draw_ginv(jax.random.fold_in(seeds[4], 71), 0),
        "rhs": scatter_about(seeds[1], (AREAS * STATE, SNAP), 1.0, 6.0, ((0, 128),), jnp.float32),
        "bnd_row": draw_bnd_row(jax.random.fold_in(seeds[4], 71), 0),
        "bnd_var": draw_bnd_var(jax.random.fold_in(seeds[4], 71), 0),
    }


PENALTY = 1.0


def solve_area(pair):
    return jnp.dot(pair[0], pair[1], preferred_element_type=jnp.float32)


def reference(ginv, rhs, bnd_row, bnd_var):
    areas_total, state_size, _ = ginv.shape
    snap_count = rhs.shape[1]
    active = (bnd_row >= 0).reshape(-1)
    offsets = (jnp.arange(areas_total, dtype=jnp.int32) * state_size)[:, None]
    rows_flat = jnp.where(bnd_row >= 0, offsets + bnd_row, 0).reshape(-1).astype(jnp.int32)
    var_safe = jnp.where(bnd_var >= 0, bnd_var, 0).reshape(-1).astype(jnp.int32)
    counts = jax.ops.segment_sum(active.astype(jnp.float32), var_safe, num_segments=VARS)
    inverse = 1.0 / jnp.maximum(counts, 1.0)
    mask = active[:, None]
    n_entries = rows_flat.shape[0]
    dual_value = jnp.zeros((n_entries, snap_count), jnp.float32)
    agreed = jnp.zeros((n_entries, snap_count), jnp.float32)
    states = None
    consensus = None
    for iteration in range(ITERS):
        shifted = jnp.where(mask, agreed - dual_value, 0.0)
        update = jnp.zeros((areas_total * state_size, snap_count), jnp.float32).at[rows_flat].add(shifted)
        blended = (rhs + PENALTY * update).astype(jnp.bfloat16).reshape(areas_total, state_size, snap_count)
        states = lax.map(solve_area, (ginv, blended)).reshape(areas_total * state_size, snap_count)
        local_part = jnp.where(mask, states[rows_flat] + dual_value, 0.0)
        totals = jax.ops.segment_sum(local_part, var_safe, num_segments=VARS)
        consensus = totals * inverse[:, None]
        agreed = jnp.where(mask, consensus[var_safe], 0.0)
        dual_value = jnp.where(mask, local_part - agreed, 0.0)
    return states, consensus, dual_value
```

```python
import jax
import jax.numpy as jnp
from jax import lax
from jax.experimental import pallas as pl
from jax.experimental.pallas import tpu as pltpu
from jax.sharding import PartitionSpec as P

SLOT = 4
VAR_DEV = 64
ITERS = 4
PENALTY = 1.0
WIDE = 8

F32 = jnp.float32
BF16 = jnp.bfloat16


def split3(x):
    hi = x.astype(BF16)
    rest = x - hi.astype(F32)
    mid = rest.astype(BF16)
    low = (rest - mid.astype(F32)).astype(BF16)
    return [hi, mid, low]


def join3(y, at=0, width=128):
    return (y[:, at : at + width] + y[:, at + width : at + 2 * width]) + y[
        :, at + 2 * width : at + 3 * width
    ]


def dot(a, b):
    return jnp.dot(a, b, preferred_element_type=F32)


def dot_t(a, b):
    return lax.dot_general(a, b, (((0,), (0,)), ((), ())), preferred_element_type=F32)


def dot_nt(a, b):
    return lax.dot_general(a, b, (((1,), (1,)), ((), ())), preferred_element_type=F32)


def iota(shape, dim):
    return lax.broadcasted_iota(jnp.int32, shape, dim)


def prepare_kernel(
    row_ref, var_ref, ginv_ref, rhs_ref,
    inner_ref, cols_ref, place_ref, mat_ref, base_ref, term_ref, local_ref, out_ref,
    carry_ref, ids_ref, acc_ref,
):
    area = pl.program_id(0)
    last = pl.num_programs(0) - 1
    bound = row_ref.shape[1]
    state = ginv_ref.shape[1]
    slots = mat_ref.shape[0]
    owners = slots // SLOT

    @pl.when(area == 0)
    def _():
        carry_ref[...] = jnp.zeros_like(carry_ref)
        ids_ref[...] = jnp.zeros_like(ids_ref)
        acc_ref[...] = jnp.zeros_like(acc_ref)
        base_ref[...] = jnp.zeros_like(base_ref)
        term_ref[...] = jnp.zeros_like(term_ref)

    row = row_ref[pl.ds(area, 1), :]
    var = var_ref[pl.ds(area, 1), :]
    live = row >= 0
    owner = jnp.where(live, lax.shift_right_arithmetic(var, 6), -1)
    local_id = jnp.where(live, (var & (VAR_DEV - 1)) + 1, 0).astype(F32)
    owned = iota((owners, bound), 0) == owner
    owned_f = owned.astype(F32)
    before = (iota((bound, bound), 0) < iota((bound, bound), 1)).astype(F32).astype(BF16)
    earlier = dot(owned_f.astype(BF16), before)
    rank = jnp.sum(jnp.where(owned, earlier + carry_ref[...], 0.0), axis=0, keepdims=True)
    carry_ref[...] += jnp.sum(owned_f, axis=1, keepdims=True)
    rank_i = rank.astype(jnp.int32)
    slot = jnp.where(live, owner * SLOT + rank_i, -1)
    place = (iota((slots, bound), 0) == slot).astype(F32).astype(BF16)
    place_ref[...] = place
    at_rank = (iota((bound, bound), 0) == rank_i).astype(F32).astype(BF16)
    ids_ref[...] += dot_nt((owned_f * local_id).astype(BF16), at_rank)

    picks_f = (iota((state, bound), 0) == row).astype(F32)
    picks = picks_f.astype(BF16)
    is_bound = jnp.sum(picks_f, axis=1, keepdims=True) > 0.0
    rhs = rhs_ref[...]
    inner = jnp.where(is_bound, 0.0, rhs).astype(BF16)
    both = dot(ginv_ref[0], jnp.concatenate([inner, picks], axis=1))
    snaps = rhs.shape[1]
    solved = both[:, :snaps]
    cols = both[:, snaps:].astype(BF16)
    inner_ref[...] = solved
    cols_ref[0] = cols
    at_rows = dot_t(picks, jnp.concatenate(split3(solved) + split3(rhs) + [cols], axis=1))
    at_slots = dot(place, at_rows.astype(BF16))
    base_ref[...] += join3(at_slots, 0, snaps)
    term_ref[...] += join3(at_slots, 3 * snaps, snaps)
    acc_ref[...] += dot_nt(at_slots[:, 6 * snaps :].astype(BF16), place)

    @pl.when(area == last)
    def _():
        mat = acc_ref[...].astype(BF16)
        mat_ref[...] = mat
        local_ref[...] = base_ref[...] + dot(mat, term_ref[...].astype(BF16))
        for k in range(SLOT):
            out_ref[pl.ds(k, owners, stride=WIDE), :] = local_ref[pl.ds(k, owners, stride=SLOT), :]
        out_ref[pl.ds(SLOT, owners, stride=WIDE), :] = ids_ref[...] - 1.0
        for k in range(SLOT + 1, WIDE):
            out_ref[pl.ds(k, owners, stride=WIDE), :] = jnp.zeros_like(ids_ref)


def average(member, inverse, stack, ret_ref):
    totals = join3(dot_t(member, jnp.concatenate(split3(stack), axis=1)))
    consensus = totals * inverse
    back = join3(dot(member, jnp.concatenate(split3(consensus), axis=1)))
    sources = back.shape[0] // SLOT
    for k in range(SLOT):
        ret_ref[pl.ds(k, sources, stride=SLOT), :] = back[k * sources : (k + 1) * sources]
    return consensus


def first_owner_kernel(in_ref, ret_ref, member_ref, inverse_ref):
    sources = in_ref.shape[0] // WIDE
    ids = in_ref[pl.ds(SLOT, sources, stride=WIDE), :].astype(jnp.int32)
    lane = iota((sources, 128), 1)
    member = jnp.concatenate(
        [(ids[:, k : k + 1] == lane).astype(F32) for k in range(SLOT)], axis=0
    ).astype(BF16)
    counts = dot_t(member, jnp.ones((member.shape[0], 128), BF16))
    inverse = 1.0 / jnp.maximum(counts, 1.0)
    member_ref[...] = member
    inverse_ref[...] = inverse
    stack = jnp.concatenate(
        [in_ref[pl.ds(k, sources, stride=WIDE), :] for k in range(SLOT)], axis=0
    )
    average(member, inverse, stack, ret_ref)


def owner_kernel(in_ref, member_ref, inverse_ref, ret_ref, cons_ref):
    sources = in_ref.shape[0] // SLOT
    stack = jnp.concatenate(
        [in_ref[pl.ds(k, sources, stride=SLOT), :] for k in range(SLOT)], axis=0
    )
    consensus = average(member_ref[...], inverse_ref[...], stack, ret_ref)
    cons_ref[...] = consensus[:VAR_DEV]


def local_kernel(agreed_ref, local_ref, term_ref, base_ref, mat_ref, new_ref, blend_ref):
    agreed = agreed_ref[...]
    dual = local_ref[...] - agreed
    blend = (term_ref[...] + PENALTY * (agreed - dual)).astype(BF16)
    blend_ref[...] = blend
    new_ref[...] = (base_ref[...] + dot(mat_ref[...], blend)) + dual


def states_kernel(inner_ref, cols_ref, place_ref, blend_ref, states_ref):
    rows = dot_t(place_ref[...], blend_ref[...]).astype(BF16)
    states_ref[...] = inner_ref[...] + dot(cols_ref[0], rows)


def dual_kernel(agreed_ref, local_ref, place_ref, dual_ref):
    dual = local_ref[...] - agreed_ref[...]
    dual_ref[...] = join3(dot_t(place_ref[...], jnp.concatenate(split3(dual), axis=1)))


def shape(dims, dtype=F32):
    return jax.ShapeDtypeStruct(dims, dtype)


def on_device(ginv, rhs, bnd_row, bnd_var):
    areas, state, _ = ginv.shape
    snaps = rhs.shape[1]
    bound = bnd_row.shape[1]
    devices = lax.axis_size("area") * lax.axis_size("tie")
    slots = devices * SLOT
    entries = areas * bound

    def whole(*dims):
        return pl.BlockSpec(dims, lambda a: (0,) * len(dims))

    inner, cols, place, mat, base, term, local, outgoing = pl.pallas_call(
        prepare_kernel,
        grid=(areas,),
        in_specs=[
            whole(areas, bound),
            whole(areas, bound),
            pl.BlockSpec((1, state, state), lambda a: (a, 0, 0)),
            pl.BlockSpec((state, snaps), lambda a: (a, 0)),
        ],
        out_specs=[
            pl.BlockSpec((state, snaps), lambda a: (a, 0)),
            pl.BlockSpec((1, state, bound), lambda a: (a, 0, 0)),
            pl.BlockSpec((slots, bound), lambda a: (0, a)),
            whole(slots, slots),
            whole(slots, snaps),
            whole(slots, snaps),
            whole(slots, snaps),
            whole(devices * WIDE, snaps),
        ],
        out_shape=[
            shape((areas * state, snaps)),
            shape((areas, state, bound), BF16),
            shape((slots, entries), BF16),
            shape((slots, slots), BF16),
            shape((slots, snaps)),
            shape((slots, snaps)),
            shape((slots, snaps)),
            shape((devices * WIDE, snaps)),
        ],
        scratch_shapes=[
            pltpu.VMEM((devices, bound), F32),
            pltpu.VMEM((devices, bound), F32),
            pltpu.VMEM((slots, slots), F32),
        ],
        compiler_params=pltpu.CompilerParams(dimension_semantics=("arbitrary",)),
        name="prepare",
    )(bnd_row, bnd_var, ginv, rhs)

    def exchange(x):
        x = x.reshape(devices, -1, snaps)
        x = lax.all_to_all(x, ("area", "tie"), split_axis=0, concat_axis=0, tiled=True)
        return x.reshape(-1, snaps)

    returning, member, inverse = pl.pallas_call(
        first_owner_kernel,
        out_shape=[shape((slots, snaps)), shape((slots, 128), BF16), shape((128, 128))],
        name="first_owner",
    )(exchange(outgoing))
    agreed = exchange(returning)
    for _ in range(1, ITERS):
        local, blend = pl.pallas_call(
            local_kernel,
            out_shape=[shape((slots, snaps)), shape((slots, snaps), BF16)],
            name="local",
        )(agreed, local, term, base, mat)
        returning, consensus = pl.pallas_call(
            owner_kernel,
            out_shape=[shape((slots, snaps)), shape((VAR_DEV, snaps))],
            name="owner",
        )(exchange(local), member, inverse)
        agreed = exchange(returning)
    states = pl.pallas_call(
        states_kernel,
        grid=(areas,),
        in_specs=[
            pl.BlockSpec((state, snaps), lambda a: (a, 0)),
            pl.BlockSpec((1, state, bound), lambda a: (a, 0, 0)),
            pl.BlockSpec((slots, bound), lambda a: (0, a)),
            whole(slots, snaps),
        ],
        out_specs=pl.BlockSpec((state, snaps), lambda a: (a, 0)),
        out_shape=shape((areas * state, snaps)),
        name="states",
    )(inner, cols, place, blend)
    dual = pl.pallas_call(
        dual_kernel, out_shape=shape((entries, snaps)), name="dual"
    )(agreed, local, place)
    return states, consensus, dual


def solution(mesh):
    both = ("area", "tie")
    return jax.shard_map(
        on_device,
        mesh=mesh,
        in_specs=(P(both, None, None), P(both, None), P(both, None), P(both, None)),
        out_specs=(P(both, None), P(both, None), P(both, None)),
        check_vma=False,
    )
```

```python
import jax
import jax.numpy as jnp
from jax import lax
from jax.experimental import pallas as pl
from jax.experimental.pallas import tpu as pltpu
from jax.sharding import PartitionSpec as P

SLOT = 4
VAR_DEV = 64
ITERS = 4
PENALTY = 1.0
WIDE = 8

F32 = jnp.float32
BF16 = jnp.bfloat16


def split3(x):
    hi = x.astype(BF16)
    rest = x - hi.astype(F32)
    mid = rest.astype(BF16)
    low = (rest - mid.astype(F32)).astype(BF16)
    return [hi, mid, low]


def join3(y, at=0, width=128):
    return (y[:, at : at + width] + y[:, at + width : at + 2 * width]) + y[
        :, at + 2 * width : at + 3 * width
    ]


def dot(a, b):
    return jnp.dot(a, b, preferred_element_type=F32)


def dot_t(a, b):
    return lax.dot_general(a, b, (((0,), (0,)), ((), ())), preferred_element_type=F32)


def dot_nt(a, b):
    return lax.dot_general(a, b, (((1,), (1,)), ((), ())), preferred_element_type=F32)


def iota(shape, dim):
    return lax.broadcasted_iota(jnp.int32, shape, dim)


def entry_slots(row, var, carry_ref, owners):
    bound = row.shape[1]
    live = row >= 0
    owner = jnp.where(live, lax.shift_right_arithmetic(var, 6), -1)
    owned = iota((owners, bound), 0) == owner
    owned_f = owned.astype(F32)
    before = (iota((bound, bound), 0) < iota((bound, bound), 1)).astype(F32).astype(BF16)
    earlier = dot(owned_f.astype(BF16), before)
    rank = jnp.sum(jnp.where(owned, earlier + carry_ref[...], 0.0), axis=0, keepdims=True)
    carry_ref[...] += jnp.sum(owned_f, axis=1, keepdims=True)
    return jnp.where(live, owner * SLOT + rank.astype(jnp.int32), -1)


def placing(slot, slots):
    return (iota((slots, slot.shape[1]), 0) == slot).astype(F32).astype(BF16)


def picking(row, state):
    bound = row.shape[1]
    down = jnp.broadcast_to(row.astype(F32), (bound, bound)).T.astype(jnp.int32)
    lane = iota((bound, bound), 1)
    parts = [(lane + at == down).astype(F32) for at in range(0, state, bound)]
    return jnp.concatenate(parts, axis=1).astype(BF16)


def start_kernel(row_ref, var_ref, ginv_ref, rhs_ref, local_ref, out_ref, carry_ref, ids_ref):
    area = pl.program_id(0)
    slots = local_ref.shape[0]
    owners = slots // SLOT

    @pl.when(area == 0)
    def _():
        carry_ref[...] = jnp.zeros_like(carry_ref)
        ids_ref[...] = jnp.zeros_like(ids_ref)
        local_ref[...] = jnp.zeros_like(local_ref)

    row = row_ref[pl.ds(area, 1), :]
    var = var_ref[pl.ds(area, 1), :]
    place = placing(entry_slots(row, var, carry_ref, owners), slots)
    local_id = jnp.where(row >= 0, (var & (VAR_DEV - 1)) + 1, 0).astype(F32)
    ids_ref[...] += dot_nt(place, jnp.broadcast_to(local_id, (128, row.shape[1])).astype(BF16))
    picks = picking(row, ginv_ref.shape[1])
    chosen = dot(picks, ginv_ref[0]).astype(BF16)
    solved = dot(chosen, rhs_ref[...].astype(BF16))
    local_ref[...] += join3(dot(place, jnp.concatenate(split3(solved), axis=1)))

    @pl.when(area == pl.num_programs(0) - 1)
    def _():
        for k in range(SLOT):
            at = pl.ds(k, owners, stride=SLOT)
            out_ref[pl.ds(k, owners, stride=WIDE), :] = local_ref[at, :]
            out_ref[pl.ds(SLOT + k, owners, stride=WIDE), :] = ids_ref[at, :]


def prepare_kernel(
    row_ref, var_ref, ginv_ref, rhs_ref,
    inner_ref, cols_ref, place_ref, mat_ref, base_ref, term_ref,
    carry_ref, acc_ref,
):
    area = pl.program_id(0)
    slots = mat_ref.shape[0]

    @pl.when(area == 0)
    def _():
        carry_ref[...] = jnp.zeros_like(carry_ref)
        acc_ref[...] = jnp.zeros_like(acc_ref)
        base_ref[...] = jnp.zeros_like(base_ref)
        term_ref[...] = jnp.zeros_like(term_ref)

    row = row_ref[pl.ds(area, 1), :]
    var = var_ref[pl.ds(area, 1), :]
    place = placing(entry_slots(row, var, carry_ref, slots // SLOT), slots)
    place_ref[...] = place
    picks_f = (iota((ginv_ref.shape[1], row.shape[1]), 0) == row).astype(F32)
    picks = picks_f.astype(BF16)
    is_bound = jnp.sum(picks_f, axis=1, keepdims=True) > 0.0
    rhs = rhs_ref[...]
    inner = jnp.where(is_bound, 0.0, rhs).astype(BF16)
    both = dot(ginv_ref[0], jnp.concatenate([inner, picks], axis=1))
    snaps = rhs.shape[1]
    solved = both[:, :snaps]
    cols = both[:, snaps:].astype(BF16)
    inner_ref[...] = solved
    cols_ref[0] = cols
    at_rows = dot_t(picks, jnp.concatenate(split3(solved) + split3(rhs) + [cols], axis=1))
    at_slots = dot(place, at_rows.astype(BF16))
    base_ref[...] += join3(at_slots, 0, snaps)
    term_ref[...] += join3(at_slots, 3 * snaps, snaps)
    acc_ref[...] += dot_nt(at_slots[:, 6 * snaps :].astype(BF16), place)

    @pl.when(area == pl.num_programs(0) - 1)
    def _():
        mat_ref[...] = acc_ref[...].astype(BF16)


def states_kernel(inner_ref, cols_ref, place_ref, blend_ref, states_ref):
    rows = dot_t(place_ref[...], blend_ref[...]).astype(BF16)
    states_ref[...] = inner_ref[...] + dot(cols_ref[0], rows)


def exact(spec, a, b):
    return jnp.einsum(spec, a, b, precision=lax.Precision.HIGHEST, preferred_element_type=F32)


def shape(dims, dtype=F32):
    return jax.ShapeDtypeStruct(dims, dtype)


def on_device(ginv, rhs, bnd_row, bnd_var):
    areas, state, _ = ginv.shape
    snaps = rhs.shape[1]
    bound = bnd_row.shape[1]
    devices = lax.axis_size("area") * lax.axis_size("tie")
    slots = devices * SLOT
    entries = areas * bound

    def whole(*dims):
        return pl.BlockSpec(dims, lambda a: (0,) * len(dims))

    in_specs = [
        whole(areas, bound),
        whole(areas, bound),
        pl.BlockSpec((1, state, state), lambda a: (a, 0, 0)),
        pl.BlockSpec((state, snaps), lambda a: (a, 0)),
    ]
    in_order = pltpu.CompilerParams(dimension_semantics=("arbitrary",))
    local, outgoing = pl.pallas_call(
        start_kernel,
        grid=(areas,),
        in_specs=in_specs,
        out_specs=[whole(slots, snaps), whole(devices * WIDE, snaps)],
        out_shape=[shape((slots, snaps)), shape((devices * WIDE, snaps))],
        scratch_shapes=[pltpu.VMEM((devices, bound), F32), pltpu.VMEM((slots, snaps), F32)],
        compiler_params=in_order,
        name="start",
    )(bnd_row, bnd_var, ginv, rhs)
    inner, cols, place, mat, base, term = pl.pallas_call(
        prepare_kernel,
        grid=(areas,),
        in_specs=in_specs,
        out_specs=[
            pl.BlockSpec((state, snaps), lambda a: (a, 0)),
            pl.BlockSpec((1, state, bound), lambda a: (a, 0, 0)),
            pl.BlockSpec((slots, bound), lambda a: (0, a)),
            whole(slots, slots),
            whole(slots, snaps),
            whole(slots, snaps),
        ],
        out_shape=[
            shape((areas * state, snaps)),
            shape((areas, state, bound), BF16),
            shape((slots, entries), BF16),
            shape((slots, slots), BF16),
            shape((slots, snaps)),
            shape((slots, snaps)),
        ],
        scratch_shapes=[pltpu.VMEM((devices, bound), F32), pltpu.VMEM((slots, slots), F32)],
        compiler_params=in_order,
        name="prepare",
    )(bnd_row, bnd_var, ginv, rhs)

    def exchange(x):
        x = x.reshape(devices, -1, snaps)
        return lax.all_to_all(x, ("area", "tie"), split_axis=0, concat_axis=0, tiled=True)

    received = exchange(outgoing)
    incoming = received[:, :SLOT].reshape(slots, snaps)
    ids = received[:, SLOT:].reshape(slots, snaps)[:, :VAR_DEV]
    member = (ids == jnp.arange(1, VAR_DEV + 1, dtype=jnp.int32).astype(F32)).astype(F32)
    inverse = 1.0 / jnp.maximum(jnp.sum(member, axis=0), 1.0)[:, None]
    for iteration in range(ITERS):
        if iteration > 0:
            blend = (term + PENALTY * (agreed - dual)).astype(BF16)
            local = (base + dot(mat, blend)) + dual
            incoming = exchange(local).reshape(slots, snaps)
        consensus = exact("sv,sn->vn", member, incoming) * inverse
        agreed = exchange(exact("sv,vn->sn", member, consensus)).reshape(slots, snaps)
        dual = local - agreed
    states = pl.pallas_call(
        states_kernel,
        grid=(areas,),
        in_specs=[
            pl.BlockSpec((state, snaps), lambda a: (a, 0)),
            pl.BlockSpec((1, state, bound), lambda a: (a, 0, 0)),
            pl.BlockSpec((slots, bound), lambda a: (0, a)),
            whole(slots, snaps),
        ],
        out_specs=pl.BlockSpec((state, snaps), lambda a: (a, 0)),
        out_shape=shape((areas * state, snaps)),
        name="states",
    )(inner, cols, place, blend)
    dual = exact("se,sn->en", place.astype(F32), dual)
    return states, consensus, dual


def solution(mesh):
    both = ("area", "tie")
    return jax.shard_map(
        on_device,
        mesh=mesh,
        in_specs=(P(both, None, None), P(both, None), P(both, None), P(both, None)),
        out_specs=(P(both, None), P(both, None), P(both, None)),
        check_vma=False,
    )
```

```python
import jax
import jax.numpy as jnp
from jax import lax
from jax.experimental import pallas as pl
from jax.experimental.pallas import tpu as pltpu
from jax.sharding import PartitionSpec as P

SLOT = 4
VAR_DEV = 64
ITERS = 4
PENALTY = 1.0
HALVES = 2
WIDE = 8

F32 = jnp.float32
BF16 = jnp.bfloat16


def split3(x):
    hi = x.astype(BF16)
    rest = x - hi.astype(F32)
    mid = rest.astype(BF16)
    low = (rest - mid.astype(F32)).astype(BF16)
    return [hi, mid, low]


def join3(y, at=0, width=128):
    return (y[:, at : at + width] + y[:, at + width : at + 2 * width]) + y[
        :, at + 2 * width : at + 3 * width
    ]


def dot(a, b):
    return jnp.dot(a, b, preferred_element_type=F32)


def dot_t(a, b):
    return lax.dot_general(a, b, (((0,), (0,)), ((), ())), preferred_element_type=F32)


def dot_nt(a, b):
    return lax.dot_general(a, b, (((1,), (1,)), ((), ())), preferred_element_type=F32)


def iota(shape, dim):
    return lax.broadcasted_iota(jnp.int32, shape, dim)


def entry_slots(row, var, carry_ref, owners):
    bound = row.shape[1]
    live = row >= 0
    owner = jnp.where(live, lax.shift_right_arithmetic(var, 6), -1)
    owned = iota((owners, bound), 0) == owner
    owned_f = owned.astype(F32)
    before = (iota((bound, bound), 0) < iota((bound, bound), 1)).astype(F32).astype(BF16)
    earlier = dot(owned_f.astype(BF16), before)
    rank = jnp.sum(jnp.where(owned, earlier + carry_ref[...], 0.0), axis=0, keepdims=True)
    carry_ref[...] += jnp.sum(owned_f, axis=1, keepdims=True)
    return jnp.where(live, owner * SLOT + rank.astype(jnp.int32), -1)


def placing(slot, slots):
    return (iota((slots, slot.shape[1]), 0) == slot).astype(F32).astype(BF16)


def picking(row, state):
    bound = row.shape[1]
    down = jnp.broadcast_to(row.astype(F32), (bound, bound)).T.astype(jnp.int32)
    lane = iota((bound, bound), 1)
    parts = [(lane + at == down).astype(F32) for at in range(0, state, bound)]
    return jnp.concatenate(parts, axis=1).astype(BF16)


def start_kernel(
    row_ref, var_ref, ginv_ref, rhs_ref, local_ref, out_ref, chosen_ref,
    block_ref, right_ref, carry_ref, block_sems, right_sems,
):
    areas = row_ref.shape[0]
    state = ginv_ref.shape[1]
    slots = local_ref.shape[0]
    owners = slots // SLOT
    half = state // HALVES

    def block_copy(area, at):
        rows = pl.ds(at * half, half)
        return pltpu.make_async_copy(
            ginv_ref.at[area, rows], block_ref.at[area, rows], block_sems.at[area * HALVES + at]
        )

    def right_copy(area):
        rows = pl.ds(area * state, state)
        return pltpu.make_async_copy(rhs_ref.at[rows], right_ref.at[rows], right_sems.at[area])

    for area in range(areas):
        for at in range(HALVES):
            block_copy(area, at).start()
        right_copy(area).start()
    carry_ref[...] = jnp.zeros_like(carry_ref)
    ids = jnp.zeros(local_ref.shape, F32)
    places = []
    picks = []
    for area in range(areas):
        row = row_ref[area : area + 1, :]
        var = var_ref[area : area + 1, :]
        places.append(placing(entry_slots(row, var, carry_ref, owners), slots))
        picks.append(picking(row, state))
        local_id = jnp.where(row >= 0, (var & (VAR_DEV - 1)) + 1, 0).astype(F32)
        ids += dot_nt(places[area], jnp.broadcast_to(local_id, (128, row.shape[1])).astype(BF16))
    local_ref[...] = ids
    for k in range(SLOT):
        at = pl.ds(k, owners, stride=SLOT)
        out_ref[pl.ds(SLOT + k, owners, stride=WIDE), :] = local_ref[at, :]
    local = jnp.zeros(local_ref.shape, F32)
    for area in range(areas):
        chosen = jnp.zeros((row_ref.shape[1], state), F32)
        for at in range(HALVES):
            block_copy(area, at).wait()
            rows = slice(at * half, (at + 1) * half)
            chosen += dot(picks[area][:, rows], block_ref[area, rows, :])
        chosen = chosen.astype(BF16)
        chosen_ref[area] = chosen
        right_copy(area).wait()
        solved = dot(chosen, right_ref[area * state : (area + 1) * state, :].astype(BF16))
        local += join3(dot(places[area], jnp.concatenate(split3(solved), axis=1)))
    local_ref[...] = local
    for k in range(SLOT):
        at = pl.ds(k, owners, stride=SLOT)
        out_ref[pl.ds(k, owners, stride=WIDE), :] = local_ref[at, :]


def prepare_kernel(
    row_ref, var_ref, chosen_ref, rhs_ref, local_ref,
    place_ref, mat_ref, base_ref, term_ref,
    carry_ref, acc_ref,
):
    area = pl.program_id(0)
    slots = mat_ref.shape[0]
    state, snaps = rhs_ref.shape

    @pl.when(area == 0)
    def _():
        carry_ref[...] = jnp.zeros_like(carry_ref)
        acc_ref[...] = jnp.zeros_like(acc_ref)
        term_ref[...] = jnp.zeros_like(term_ref)

    row = row_ref[pl.ds(area, 1), :]
    var = var_ref[pl.ds(area, 1), :]
    place = placing(entry_slots(row, var, carry_ref, slots // SLOT), slots)
    place_ref[...] = place
    at_rows = dot(picking(row, state), jnp.concatenate(split3(rhs_ref[...]), axis=1))
    coupling = dot(chosen_ref[0], placing(row, state))
    at_slots = dot(place, jnp.concatenate([at_rows, coupling], axis=1).astype(BF16))
    term_ref[...] += join3(at_slots, 0, snaps)
    acc_ref[...] += dot_nt(at_slots[:, 3 * snaps :].astype(BF16), place)

    @pl.when(area == pl.num_programs(0) - 1)
    def _():
        mat = acc_ref[...].astype(BF16)
        mat_ref[...] = mat
        base_ref[...] = local_ref[...] - dot(mat, term_ref[...].astype(BF16))


def states_kernel(row_ref, ginv_ref, rhs_ref, place_ref, blend_ref, states_ref):
    row = row_ref[pl.ds(pl.program_id(0), 1), :]
    state, snaps = rhs_ref.shape
    rows = dot_t(place_ref[...], blend_ref[...]).astype(BF16)
    placed = dot(placing(row, state), jnp.concatenate([rows, jnp.ones_like(rows)], axis=1))
    blended = jnp.where(placed[:, snaps:] > 0.0, placed[:, :snaps], rhs_ref[...])
    states_ref[...] = dot(ginv_ref[0], blended.astype(BF16))


def exact(spec, a, b):
    return jnp.einsum(spec, a, b, precision=lax.Precision.HIGHEST, preferred_element_type=F32)


def shape(dims, dtype=F32):
    return jax.ShapeDtypeStruct(dims, dtype)


def on_device(ginv, rhs, bnd_row, bnd_var):
    areas, state, _ = ginv.shape
    snaps = rhs.shape[1]
    bound = bnd_row.shape[1]
    devices = lax.axis_size("area") * lax.axis_size("tie")
    slots = devices * SLOT
    entries = areas * bound

    def whole(*dims):
        return pl.BlockSpec(dims, lambda a: (0,) * len(dims))

    in_order = pltpu.CompilerParams(dimension_semantics=("arbitrary",))
    anywhere = pl.BlockSpec(memory_space=pl.ANY)
    small = pl.BlockSpec((areas, bound), lambda: (0, 0))
    local, outgoing, chosen = pl.pallas_call(
        start_kernel,
        in_specs=[small, small, anywhere, anywhere],
        out_shape=[
            pltpu.VMEM((slots, snaps), F32),
            pltpu.VMEM((devices * WIDE, snaps), F32),
            pltpu.VMEM((areas, bound, state), BF16),
        ],
        scratch_shapes=[
            pltpu.VMEM((areas, state, state), BF16),
            pltpu.VMEM((areas * state, snaps), F32),
            pltpu.VMEM((devices, bound), F32),
            pltpu.SemaphoreType.DMA((areas * HALVES,)),
            pltpu.SemaphoreType.DMA((areas,)),
        ],
        name="start",
    )(bnd_row, bnd_var, ginv, rhs)
    place, mat, base, term = pl.pallas_call(
        prepare_kernel,
        grid=(areas,),
        in_specs=[
            whole(areas, bound),
            whole(areas, bound),
            pl.BlockSpec((1, bound, state), lambda a: (a, 0, 0)),
            pl.BlockSpec((state, snaps), lambda a: (a, 0)),
            whole(slots, snaps),
        ],
        out_specs=[
            pl.BlockSpec((slots, bound), lambda a: (0, a)),
            whole(slots, slots),
            whole(slots, snaps),
            whole(slots, snaps),
        ],
        out_shape=[
            pltpu.VMEM((slots, entries), BF16),
            pltpu.VMEM((slots, slots), BF16),
            pltpu.VMEM((slots, snaps), F32),
            pltpu.VMEM((slots, snaps), F32),
        ],
        scratch_shapes=[pltpu.VMEM((devices, bound), F32), pltpu.VMEM((slots, slots), F32)],
        compiler_params=in_order,
        name="prepare",
    )(bnd_row, bnd_var, chosen, rhs, local)

    def exchange(x):
        x = x.reshape(devices, -1, snaps)
        return lax.all_to_all(x, ("area", "tie"), split_axis=0, concat_axis=0, tiled=True)

    received, place, mat, base, term = lax.optimization_barrier(
        (exchange(outgoing), place, mat, base, term)
    )
    incoming = received[:, :SLOT].reshape(slots, snaps)
    ids = received[:, SLOT:].reshape(slots, snaps)[:, :VAR_DEV]
    member = (ids == jnp.arange(1, VAR_DEV + 1, dtype=jnp.int32).astype(F32)).astype(F32)
    inverse = 1.0 / jnp.maximum(jnp.sum(member, axis=0), 1.0)[:, None]
    for iteration in range(ITERS):
        if iteration > 0:
            blend = (term + PENALTY * (agreed - dual)).astype(BF16)
            local = (base + dot(mat, blend)) + dual
            incoming = exchange(local).reshape(slots, snaps)
        consensus = exact("sv,sn->vn", member, incoming) * inverse
        agreed = exchange(exact("sv,vn->sn", member, consensus)).reshape(slots, snaps)
        dual = local - agreed
    states = pl.pallas_call(
        states_kernel,
        grid=(areas,),
        in_specs=[
            whole(areas, bound),
            pl.BlockSpec((1, state, state), lambda a: (a, 0, 0)),
            pl.BlockSpec((state, snaps), lambda a: (a, 0)),
            pl.BlockSpec((slots, bound), lambda a: (0, a)),
            whole(slots, snaps),
        ],
        out_specs=pl.BlockSpec((state, snaps), lambda a: (a, 0)),
        out_shape=shape((areas * state, snaps)),
        compiler_params=in_order,
        name="states",
    )(bnd_row, ginv, rhs, place, blend)
    dual = exact("se,sn->en", place.astype(F32), dual)
    return states, consensus, dual


def solution(mesh):
    both = ("area", "tie")
    return jax.shard_map(
        on_device,
        mesh=mesh,
        in_specs=(P(both, None, None), P(both, None), P(both, None), P(both, None)),
        out_specs=(P(both, None), P(both, None), P(both, None)),
        check_vma=False,
    )
```

```python
import jax
import jax.numpy as jnp
from jax import lax
from jax.experimental import pallas as pl
from jax.experimental.pallas import tpu as pltpu
from jax.sharding import PartitionSpec as P

SLOT = 4
VAR_DEV = 64
ITERS = 4
PENALTY = 1.0
PIECE = 128
BUILD = 256
WIDE = 8

F32 = jnp.float32
BF16 = jnp.bfloat16


def split3(x):
    hi = x.astype(BF16)
    rest = x - hi.astype(F32)
    mid = rest.astype(BF16)
    low = (rest - mid.astype(F32)).astype(BF16)
    return [hi, mid, low]


def join3(y, at=0, width=128):
    return (y[:, at : at + width] + y[:, at + width : at + 2 * width]) + y[
        :, at + 2 * width : at + 3 * width
    ]


def dot(a, b):
    return jnp.dot(a, b, preferred_element_type=F32)


def dot_t(a, b):
    return lax.dot_general(a, b, (((0,), (0,)), ((), ())), preferred_element_type=F32)


def dot_nt(a, b):
    return lax.dot_general(a, b, (((1,), (1,)), ((), ())), preferred_element_type=F32)


def iota(shape, dim):
    return lax.broadcasted_iota(jnp.int32, shape, dim)


def entry_slots(row, var, carry_ref, owners):
    bound = row.shape[1]
    live = row >= 0
    owner = jnp.where(live, lax.shift_right_arithmetic(var, 6), -1)
    owned = iota((owners, bound), 0) == owner
    owned_f = owned.astype(F32)
    before = (iota((bound, bound), 0) < iota((bound, bound), 1)).astype(F32).astype(BF16)
    earlier = dot(owned_f.astype(BF16), before)
    rank = jnp.sum(jnp.where(owned, earlier + carry_ref[...], 0.0), axis=0, keepdims=True)
    carry_ref[...] += jnp.sum(owned_f, axis=1, keepdims=True)
    return jnp.where(live, owner * SLOT + rank.astype(jnp.int32), -1)


def placing(slot, slots):
    return (iota((slots, slot.shape[1]), 0) == slot).astype(F32).astype(BF16)


def picking(row, state):
    bound = row.shape[1]
    down = jnp.broadcast_to(row.astype(F32), (bound, bound)).T.astype(jnp.int32)
    lane = iota((bound, bound), 1)
    parts = [(lane + at == down).astype(F32) for at in range(0, state, bound)]
    return jnp.concatenate(parts, axis=1).astype(BF16)


def start_kernel(
    row_ref, var_ref, ginv_ref, rhs_ref, local_ref, out_ref, chosen_ref,
    block_ref, right_ref, carry_ref, place_ref, solved_ref, block_sems, right_sems,
):
    areas, bound = row_ref.shape
    state = ginv_ref.shape[1]
    slots, snaps = local_ref.shape
    owners = slots // SLOT

    def block_copy(area):
        return pltpu.make_async_copy(ginv_ref.at[area], block_ref.at[area], block_sems.at[area])

    def right_copy(area):
        rows = pl.ds(area * state, state)
        return pltpu.make_async_copy(rhs_ref.at[rows], right_ref.at[rows], right_sems.at[area])

    for area in range(areas):
        block_copy(area).start()
        right_copy(area).start()
    carry_ref[...] = jnp.zeros_like(carry_ref)
    picks = []
    local_ids = []
    for area in range(areas):
        row = row_ref[area : area + 1, :]
        var = var_ref[area : area + 1, :]
        place_ref[:, area * bound : (area + 1) * bound] = placing(
            entry_slots(row, var, carry_ref, owners), slots
        )
        picks.append(picking(row, state))
        local_ids.append(jnp.where(row >= 0, (var & (VAR_DEV - 1)) + 1, 0).astype(F32))
    local_ids = jnp.broadcast_to(jnp.concatenate(local_ids, axis=1), (128, areas * bound))
    local_ref[...] = dot_nt(place_ref[...], local_ids.astype(BF16))
    for k in range(SLOT):
        at = pl.ds(k, owners, stride=SLOT)
        out_ref[pl.ds(SLOT + k, owners, stride=WIDE), :] = local_ref[at, :]
    for area in range(areas):
        block_copy(area).wait()
        right_copy(area).wait()
        chosen = dot(picks[area], block_ref[area]).astype(BF16)
        chosen_ref[area] = chosen
        solved = dot(chosen, right_ref[area * state : (area + 1) * state, :].astype(BF16))
        solved_ref[area * bound : (area + 1) * bound, :] = jnp.concatenate(split3(solved), axis=1)
    local_ref[...] = join3(dot(place_ref[...], solved_ref[...]), 0, snaps)
    for k in range(SLOT):
        at = pl.ds(k, owners, stride=SLOT)
        out_ref[pl.ds(k, owners, stride=WIDE), :] = local_ref[at, :]


def prepare_kernel(
    row_ref, var_ref, chosen_ref, rhs_ref,
    place_ref, mat_ref, term_ref,
    carry_ref, acc_ref,
):
    area = pl.program_id(0)
    slots = mat_ref.shape[0]
    state, snaps = rhs_ref.shape

    @pl.when(area == 0)
    def _():
        carry_ref[...] = jnp.zeros_like(carry_ref)
        acc_ref[...] = jnp.zeros_like(acc_ref)
        term_ref[...] = jnp.zeros_like(term_ref)

    row = row_ref[pl.ds(area, 1), :]
    var = var_ref[pl.ds(area, 1), :]
    place = placing(entry_slots(row, var, carry_ref, slots // SLOT), slots)
    place_ref[...] = place
    at_rows = dot(picking(row, state), jnp.concatenate(split3(rhs_ref[...]), axis=1))
    coupling = dot(chosen_ref[0], placing(row, state))
    at_slots = dot(place, jnp.concatenate([at_rows, coupling], axis=1).astype(BF16))
    term_ref[...] += join3(at_slots, 0, snaps)
    acc_ref[...] += dot_nt(at_slots[:, 3 * snaps :].astype(BF16), place)

    @pl.when(area == pl.num_programs(0) - 1)
    def _():
        mat_ref[...] = acc_ref[...].astype(BF16)


def states_kernel(
    row_ref, ginv_ref, rhs_ref, place_ref, blend_ref, states_ref,
    block_ref, right_ref, solved_ref, block_sems, right_sems, out_sems,
):
    areas, bound = row_ref.shape
    state = ginv_ref.shape[1]
    snaps = rhs_ref.shape[1]

    def rows_of(area):
        return pl.ds(area * state, state)

    def right_copy(area):
        rows = rows_of(area)
        return pltpu.make_async_copy(rhs_ref.at[rows], right_ref.at[rows], right_sems.at[area])

    def block_copy(area):
        return pltpu.make_async_copy(ginv_ref.at[area], block_ref.at[area], block_sems.at[area])

    def out_copy(area):
        rows = rows_of(area)
        return pltpu.make_async_copy(solved_ref.at[rows], states_ref.at[rows], out_sems.at[area])

    for area in range(areas):
        right_copy(area).start()
        block_copy(area).start()
    entry_rows = dot_t(place_ref[...], blend_ref[...]).astype(BF16)
    for area in range(areas):
        row = row_ref[area : area + 1, :]
        rows = entry_rows[area * bound : (area + 1) * bound]
        both = jnp.concatenate([rows, jnp.ones_like(rows)], axis=1)
        right_copy(area).wait()
        pieces = []
        for at in range(0, state, BUILD):
            placed = dot(placing(row - at, BUILD), both)
            right = right_ref[area * state + at : area * state + at + BUILD, :]
            piece = jnp.where(placed[:, snaps:] > 0.0, placed[:, :snaps], right)
            pieces.append(piece.astype(BF16))
        blended = jnp.concatenate(pieces, axis=0)
        block_copy(area).wait()
        for at in range(0, state, PIECE):
            solved = dot(block_ref[area, at : at + PIECE, :], blended)
            solved_ref[area * state + at : area * state + at + PIECE, :] = solved
        out_copy(area).start()
    for area in range(areas):
        out_copy(area).wait()


def exact(spec, a, b):
    return jnp.einsum(spec, a, b, precision=lax.Precision.HIGHEST, preferred_element_type=F32)


def shape(dims, dtype=F32):
    return jax.ShapeDtypeStruct(dims, dtype)


def on_device(ginv, rhs, bnd_row, bnd_var):
    areas, state, _ = ginv.shape
    snaps = rhs.shape[1]
    bound = bnd_row.shape[1]
    devices = lax.axis_size("area") * lax.axis_size("tie")
    slots = devices * SLOT
    entries = areas * bound

    def whole(*dims):
        return pl.BlockSpec(dims, lambda a: (0,) * len(dims))

    in_order = pltpu.CompilerParams(dimension_semantics=("arbitrary",))
    anywhere = pl.BlockSpec(memory_space=pl.ANY)
    small = pl.BlockSpec((areas, bound), lambda: (0, 0))
    local, outgoing, chosen = pl.pallas_call(
        start_kernel,
        in_specs=[small, small, anywhere, anywhere],
        out_shape=[
            pltpu.VMEM((slots, snaps), F32),
            pltpu.VMEM((devices * WIDE, snaps), F32),
            pltpu.VMEM((areas, bound, state), BF16),
        ],
        scratch_shapes=[
            pltpu.VMEM((areas, state, state), BF16),
            pltpu.VMEM((areas * state, snaps), F32),
            pltpu.VMEM((devices, bound), F32),
            pltpu.VMEM((slots, entries), BF16),
            pltpu.VMEM((entries, 3 * snaps), BF16),
            pltpu.SemaphoreType.DMA((areas,)),
            pltpu.SemaphoreType.DMA((areas,)),
        ],
        name="start",
    )(bnd_row, bnd_var, ginv, rhs)
    place, mat, term = pl.pallas_call(
        prepare_kernel,
        grid=(areas,),
        in_specs=[
            whole(areas, bound),
            whole(areas, bound),
            pl.BlockSpec((1, bound, state), lambda a: (a, 0, 0)),
            pl.BlockSpec((state, snaps), lambda a: (a, 0)),
        ],
        out_specs=[
            pl.BlockSpec((slots, bound), lambda a: (0, a)),
            whole(slots, slots),
            whole(slots, snaps),
        ],
        out_shape=[
            pltpu.VMEM((slots, entries), BF16),
            pltpu.VMEM((slots, slots), BF16),
            pltpu.VMEM((slots, snaps), F32),
        ],
        scratch_shapes=[pltpu.VMEM((devices, bound), F32), pltpu.VMEM((slots, slots), F32)],
        compiler_params=in_order,
        name="prepare",
    )(bnd_row, bnd_var, chosen, rhs)

    def exchange(x):
        x = x.reshape(devices, -1, snaps)
        return lax.all_to_all(x, ("area", "tie"), split_axis=0, concat_axis=0, tiled=True)

    base = local - dot(mat, term.astype(BF16))
    received, place, mat, base, term = lax.optimization_barrier(
        (exchange(outgoing), place, mat, base, term)
    )
    incoming = received[:, :SLOT].reshape(slots, snaps)
    ids = received[:, SLOT:].reshape(slots, snaps)[:, :VAR_DEV]
    member = (ids == jnp.arange(1, VAR_DEV + 1, dtype=jnp.int32).astype(F32)).astype(F32)
    inverse = 1.0 / jnp.maximum(jnp.sum(member, axis=0), 1.0)[:, None]
    for iteration in range(ITERS):
        if iteration > 0:
            blend = (term + PENALTY * (agreed - dual)).astype(BF16)
            local = (base + dot(mat, blend)) + dual
            incoming = exchange(local).reshape(slots, snaps)
        consensus = exact("sv,sn->vn", member, incoming) * inverse
        agreed = exchange(exact("sv,vn->sn", member, consensus)).reshape(slots, snaps)
        dual = local - agreed
    states = pl.pallas_call(
        states_kernel,
        in_specs=[
            small,
            anywhere,
            anywhere,
            pl.BlockSpec((slots, entries), lambda: (0, 0)),
            pl.BlockSpec((slots, snaps), lambda: (0, 0)),
        ],
        out_specs=anywhere,
        out_shape=shape((areas * state, snaps)),
        scratch_shapes=[
            pltpu.VMEM((areas, state, state), BF16),
            pltpu.VMEM((areas * state, snaps), F32),
            pltpu.VMEM((areas * state, snaps), F32),
            pltpu.SemaphoreType.DMA((areas,)),
            pltpu.SemaphoreType.DMA((areas,)),
            pltpu.SemaphoreType.DMA((areas,)),
        ],
        name="states",
    )(bnd_row, ginv, rhs, place, blend)
    dual = exact("se,sn->en", place.astype(F32), dual)
    return states, consensus, dual


def solution(mesh):
    both = ("area", "tie")
    return jax.shard_map(
        on_device,
        mesh=mesh,
        in_specs=(P(both, None, None), P(both, None), P(both, None), P(both, None)),
        out_specs=(P(both, None), P(both, None), P(both, None)),
        check_vma=False,
    )
```

```python
import jax
import jax.numpy as jnp
from jax import lax
from jax.experimental import pallas as pl
from jax.experimental.pallas import tpu as pltpu
from jax.sharding import PartitionSpec as P

SLOT = 4
VAR_DEV = 64
ITERS = 4
PENALTY = 1.0
PIECE = 128
BUILD = 256
WIDE = 8

F32 = jnp.float32
BF16 = jnp.bfloat16


def split3(x):
    hi = x.astype(BF16)
    rest = x - hi.astype(F32)
    mid = rest.astype(BF16)
    low = (rest - mid.astype(F32)).astype(BF16)
    return [hi, mid, low]


def join3(y, at=0, width=128):
    return (y[:, at : at + width] + y[:, at + width : at + 2 * width]) + y[
        :, at + 2 * width : at + 3 * width
    ]


def dot(a, b):
    return jnp.dot(a, b, preferred_element_type=F32)


def dot_t(a, b):
    return lax.dot_general(a, b, (((0,), (0,)), ((), ())), preferred_element_type=F32)


def dot_nt(a, b):
    return lax.dot_general(a, b, (((1,), (1,)), ((), ())), preferred_element_type=F32)


def iota(shape, dim):
    return lax.broadcasted_iota(jnp.int32, shape, dim)


def entry_slots(row, var, carry_ref, owners):
    bound = row.shape[1]
    live = row >= 0
    owner = jnp.where(live, lax.shift_right_arithmetic(var, 6), -1)
    owned = iota((owners, bound), 0) == owner
    owned_f = owned.astype(F32)
    before = (iota((bound, bound), 0) < iota((bound, bound), 1)).astype(F32).astype(BF16)
    earlier = dot(owned_f.astype(BF16), before)
    rank = jnp.sum(jnp.where(owned, earlier + carry_ref[...], 0.0), axis=0, keepdims=True)
    carry_ref[...] += jnp.sum(owned_f, axis=1, keepdims=True)
    return jnp.where(live, owner * SLOT + rank.astype(jnp.int32), -1)


def placing(slot, slots):
    return (iota((slots, slot.shape[1]), 0) == slot).astype(F32).astype(BF16)


def picking(row, state):
    bound = row.shape[1]
    down = jnp.broadcast_to(row.astype(F32), (bound, bound)).T.astype(jnp.int32)
    lane = iota((bound, bound), 1)
    parts = [(lane + at == down).astype(F32) for at in range(0, state, bound)]
    return jnp.concatenate(parts, axis=1).astype(BF16)


def start_kernel(
    row_ref, var_ref, ginv_ref, rhs_ref, local_ref, out_ref, chosen_ref,
    block_ref, right_ref, carry_ref, place_ref, solved_ref, block_sems, right_sems,
):
    areas, bound = row_ref.shape
    state = ginv_ref.shape[1]
    slots, snaps = local_ref.shape
    owners = slots // SLOT

    def block_copy(area):
        return pltpu.make_async_copy(ginv_ref.at[area], block_ref.at[area], block_sems.at[area])

    def right_copy(area):
        rows = pl.ds(area * state, state)
        return pltpu.make_async_copy(rhs_ref.at[rows], right_ref.at[rows], right_sems.at[area])

    for area in range(areas):
        block_copy(area).start()
        right_copy(area).start()
    carry_ref[...] = jnp.zeros_like(carry_ref)
    picks = []
    local_ids = []
    for area in range(areas):
        row = row_ref[area : area + 1, :]
        var = var_ref[area : area + 1, :]
        place_ref[:, area * bound : (area + 1) * bound] = placing(
            entry_slots(row, var, carry_ref, owners), slots
        )
        picks.append(picking(row, state))
        local_ids.append(jnp.where(row >= 0, (var & (VAR_DEV - 1)) + 1, 0).astype(F32))
    local_ids = jnp.broadcast_to(jnp.concatenate(local_ids, axis=1), (128, areas * bound))
    local_ref[...] = dot_nt(place_ref[...], local_ids.astype(BF16))
    for k in range(SLOT):
        at = pl.ds(k, owners, stride=SLOT)
        out_ref[pl.ds(SLOT + k, owners, stride=WIDE), :] = local_ref[at, :]
    for area in range(areas):
        block_copy(area).wait()
        right_copy(area).wait()
        chosen = dot(picks[area], block_ref[area]).astype(BF16)
        chosen_ref[area] = chosen
        solved = dot(chosen, right_ref[area * state : (area + 1) * state, :].astype(BF16))
        solved_ref[area * bound : (area + 1) * bound, :] = jnp.concatenate(split3(solved), axis=1)
    local_ref[...] = join3(dot(place_ref[...], solved_ref[...]), 0, snaps)
    for k in range(SLOT):
        at = pl.ds(k, owners, stride=SLOT)
        out_ref[pl.ds(k, owners, stride=WIDE), :] = local_ref[at, :]


def prepare_kernel(
    row_ref, var_ref, chosen_ref, rhs_ref,
    place_ref, mat_ref, term_ref, inner_ref,
    carry_ref, acc_ref,
):
    area = pl.program_id(0)
    slots = mat_ref.shape[0]
    state, snaps = rhs_ref.shape

    @pl.when(area == 0)
    def _():
        carry_ref[...] = jnp.zeros_like(carry_ref)
        acc_ref[...] = jnp.zeros_like(acc_ref)
        term_ref[...] = jnp.zeros_like(term_ref)

    row = row_ref[pl.ds(area, 1), :]
    var = var_ref[pl.ds(area, 1), :]
    place = placing(entry_slots(row, var, carry_ref, slots // SLOT), slots)
    place_ref[...] = place
    for at in range(0, state, BUILD):
        bound_rows = dot(placing(row - at, BUILD), jnp.ones((row.shape[1], snaps), BF16)) > 0.0
        inner_ref[at : at + BUILD, :] = jnp.where(
            bound_rows, 0.0, rhs_ref[at : at + BUILD, :]
        ).astype(BF16)
    at_rows = dot(picking(row, state), jnp.concatenate(split3(rhs_ref[...]), axis=1))
    coupling = dot(chosen_ref[0], placing(row, state))
    at_slots = dot(place, jnp.concatenate([at_rows, coupling], axis=1).astype(BF16))
    term_ref[...] += join3(at_slots, 0, snaps)
    acc_ref[...] += dot_nt(at_slots[:, 3 * snaps :].astype(BF16), place)

    @pl.when(area == pl.num_programs(0) - 1)
    def _():
        mat_ref[...] = acc_ref[...].astype(BF16)


def states_kernel(
    row_ref, ginv_ref, inner_ref, place_ref, blend_ref, states_ref,
    block_ref, right_ref, solved_ref, block_sems, right_sems, out_sems,
):
    areas, bound = row_ref.shape
    state = ginv_ref.shape[1]

    def rows_of(area):
        return pl.ds(area * state, state)

    def right_copy(area):
        rows = rows_of(area)
        return pltpu.make_async_copy(inner_ref.at[rows], right_ref.at[rows], right_sems.at[area])

    def block_copy(area):
        return pltpu.make_async_copy(ginv_ref.at[area], block_ref.at[area], block_sems.at[area])

    def out_copy(area):
        rows = rows_of(area)
        return pltpu.make_async_copy(solved_ref.at[rows], states_ref.at[rows], out_sems.at[area])

    for area in range(areas):
        right_copy(area).start()
        block_copy(area).start()
    entry_rows = dot_t(place_ref[...], blend_ref[...]).astype(BF16)
    for area in range(areas):
        row = row_ref[area : area + 1, :]
        rows = entry_rows[area * bound : (area + 1) * bound]
        right_copy(area).wait()
        pieces = []
        for at in range(0, state, BUILD):
            placed = dot(placing(row - at, BUILD), rows).astype(BF16)
            pieces.append(right_ref[area * state + at : area * state + at + BUILD, :] + placed)
        blended = jnp.concatenate(pieces, axis=0)
        block_copy(area).wait()
        for at in range(0, state, PIECE):
            solved = dot(block_ref[area, at : at + PIECE, :], blended)
            solved_ref[area * state + at : area * state + at + PIECE, :] = solved
        out_copy(area).start()
    for area in range(areas):
        out_copy(area).wait()


def select(spec, a, b):
    return jnp.einsum(spec, a, b, precision=lax.Precision.HIGH, preferred_element_type=F32)


def shape(dims, dtype=F32):
    return jax.ShapeDtypeStruct(dims, dtype)


def on_device(ginv, rhs, bnd_row, bnd_var):
    areas, state, _ = ginv.shape
    snaps = rhs.shape[1]
    bound = bnd_row.shape[1]
    devices = lax.axis_size("area") * lax.axis_size("tie")
    slots = devices * SLOT
    entries = areas * bound

    def whole(*dims):
        return pl.BlockSpec(dims, lambda a: (0,) * len(dims))

    in_order = pltpu.CompilerParams(dimension_semantics=("arbitrary",))
    anywhere = pl.BlockSpec(memory_space=pl.ANY)
    small = pl.BlockSpec((areas, bound), lambda: (0, 0))
    local, outgoing, chosen = pl.pallas_call(
        start_kernel,
        in_specs=[small, small, anywhere, anywhere],
        out_shape=[
            pltpu.VMEM((slots, snaps), F32),
            pltpu.VMEM((devices * WIDE, snaps), F32),
            pltpu.VMEM((areas, bound, state), BF16),
        ],
        scratch_shapes=[
            pltpu.VMEM((areas, state, state), BF16),
            pltpu.VMEM((areas * state, snaps), F32),
            pltpu.VMEM((devices, bound), F32),
            pltpu.VMEM((slots, entries), BF16),
            pltpu.VMEM((entries, 3 * snaps), BF16),
            pltpu.SemaphoreType.DMA((areas,)),
            pltpu.SemaphoreType.DMA((areas,)),
        ],
        name="start",
    )(bnd_row, bnd_var, ginv, rhs)
    place, mat, term, inner = pl.pallas_call(
        prepare_kernel,
        grid=(areas,),
        in_specs=[
            whole(areas, bound),
            whole(areas, bound),
            pl.BlockSpec((1, bound, state), lambda a: (a, 0, 0)),
            pl.BlockSpec((state, snaps), lambda a: (a, 0)),
        ],
        out_specs=[
            pl.BlockSpec((slots, bound), lambda a: (0, a)),
            whole(slots, slots),
            whole(slots, snaps),
            pl.BlockSpec((state, snaps), lambda a: (a, 0)),
        ],
        out_shape=[
            pltpu.VMEM((slots, entries), BF16),
            pltpu.VMEM((slots, slots), BF16),
            pltpu.VMEM((slots, snaps), F32),
            shape((areas * state, snaps), BF16),
        ],
        scratch_shapes=[pltpu.VMEM((devices, bound), F32), pltpu.VMEM((slots, slots), F32)],
        compiler_params=in_order,
        name="prepare",
    )(bnd_row, bnd_var, chosen, rhs)

    def exchange(x):
        x = x.reshape(devices, -1, snaps)
        return lax.all_to_all(x, ("area", "tie"), split_axis=0, concat_axis=0, tiled=True)

    base = local - dot(mat, term.astype(BF16))
    received, place, mat, base, term, inner = lax.optimization_barrier(
        (exchange(outgoing), place, mat, base, term, inner)
    )
    incoming = received[:, :SLOT].reshape(slots, snaps)
    ids = received[:, SLOT:].reshape(slots, snaps)[:, :VAR_DEV]
    member = (ids == jnp.arange(1, VAR_DEV + 1, dtype=jnp.int32).astype(F32)).astype(F32)
    inverse = 1.0 / jnp.maximum(jnp.sum(member, axis=0), 1.0)[:, None]
    for iteration in range(ITERS):
        if iteration > 0:
            blend = (term + PENALTY * (agreed - dual)).astype(BF16)
            local = (base + dot(mat, blend)) + dual
            incoming = exchange(local).reshape(slots, snaps)
        consensus = select("sv,sn->vn", member, incoming) * inverse
        agreed = exchange(select("sv,vn->sn", member, consensus)).reshape(slots, snaps)
        dual = local - agreed
    states = pl.pallas_call(
        states_kernel,
        in_specs=[
            small,
            anywhere,
            anywhere,
            pl.BlockSpec((slots, entries), lambda: (0, 0)),
            pl.BlockSpec((slots, snaps), lambda: (0, 0)),
        ],
        out_specs=anywhere,
        out_shape=shape((areas * state, snaps)),
        scratch_shapes=[
            pltpu.VMEM((areas, state, state), BF16),
            pltpu.VMEM((areas * state, snaps), BF16),
            pltpu.VMEM((areas * state, snaps), F32),
            pltpu.SemaphoreType.DMA((areas,)),
            pltpu.SemaphoreType.DMA((areas,)),
            pltpu.SemaphoreType.DMA((areas,)),
        ],
        name="states",
    )(bnd_row, ginv, inner, place, blend)
    dual = select("se,sn->en", place.astype(F32), dual)
    return states, consensus, dual


def solution(mesh):
    both = ("area", "tie")
    return jax.shard_map(
        on_device,
        mesh=mesh,
        in_specs=(P(both, None, None), P(both, None), P(both, None), P(both, None)),
        out_specs=(P(both, None), P(both, None), P(both, None)),
        check_vma=False,
    )
```

```python
import jax
import jax.numpy as jnp
from jax import lax
from jax.experimental import pallas as pl
from jax.experimental.pallas import tpu as pltpu
from jax.sharding import PartitionSpec as P

SLOT = 4
VAR_DEV = 64
ITERS = 4
PENALTY = 1.0
PIECE = 128
BUILD = 256
WIDE = SLOT + 1

F32 = jnp.float32
BF16 = jnp.bfloat16


def split3(x):
    hi = x.astype(BF16)
    rest = x - hi.astype(F32)
    mid = rest.astype(BF16)
    low = (rest - mid.astype(F32)).astype(BF16)
    return [hi, mid, low]


def join3(y, at=0, width=128):
    return (y[:, at : at + width] + y[:, at + width : at + 2 * width]) + y[
        :, at + 2 * width : at + 3 * width
    ]


def dot(a, b):
    return jnp.dot(a, b, preferred_element_type=F32)


def dot_t(a, b):
    return lax.dot_general(a, b, (((0,), (0,)), ((), ())), preferred_element_type=F32)


def dot_nt(a, b):
    return lax.dot_general(a, b, (((1,), (1,)), ((), ())), preferred_element_type=F32)


def iota(shape, dim):
    return lax.broadcasted_iota(jnp.int32, shape, dim)


def entry_slots(row, var, carry_ref, owners):
    bound = row.shape[1]
    live = row >= 0
    owner = jnp.where(live, lax.shift_right_arithmetic(var, 6), -1)
    owned = iota((owners, bound), 0) == owner
    owned_f = owned.astype(F32)
    before = (iota((bound, bound), 0) < iota((bound, bound), 1)).astype(F32).astype(BF16)
    earlier = dot(owned_f.astype(BF16), before)
    rank = jnp.sum(jnp.where(owned, earlier + carry_ref[...], 0.0), axis=0, keepdims=True)
    carry_ref[...] += jnp.sum(owned_f, axis=1, keepdims=True)
    return jnp.where(live, owner * SLOT + rank.astype(jnp.int32), -1)


def placing(slot, slots):
    return (iota((slots, slot.shape[1]), 0) == slot).astype(F32).astype(BF16)


def picking(row, state):
    bound = row.shape[1]
    down = jnp.broadcast_to(row.astype(F32), (bound, bound)).T.astype(jnp.int32)
    lane = iota((bound, bound), 1)
    parts = [(lane + at == down).astype(F32) for at in range(0, state, bound)]
    return jnp.concatenate(parts, axis=1).astype(BF16)


def start_kernel(
    row_ref, var_ref, ginv_ref, rhs_ref, local_ref, out_ref, chosen_ref,
    block_ref, right_ref, carry_ref, place_ref, solved_ref, block_sems, right_sems,
):
    areas, bound = row_ref.shape
    state = ginv_ref.shape[1]
    slots, snaps = local_ref.shape
    owners = slots // SLOT

    def block_copy(area):
        return pltpu.make_async_copy(ginv_ref.at[area], block_ref.at[area], block_sems.at[area])

    def right_copy(area):
        rows = pl.ds(area * state, state)
        return pltpu.make_async_copy(rhs_ref.at[rows], right_ref.at[rows], right_sems.at[area])

    for area in range(areas):
        block_copy(area).start()
        right_copy(area).start()
    carry_ref[...] = jnp.zeros_like(carry_ref)
    picks = []
    local_ids = []
    for area in range(areas):
        row = row_ref[area : area + 1, :]
        var = var_ref[area : area + 1, :]
        place_ref[:, area * bound : (area + 1) * bound] = placing(
            entry_slots(row, var, carry_ref, owners), slots
        )
        picks.append(picking(row, state))
        local_ids.append(jnp.where(row >= 0, (var & (VAR_DEV - 1)) + 1, 0).astype(F32))
    local_ids = jnp.broadcast_to(jnp.concatenate(local_ids, axis=1), (128, areas * bound))
    local_ref[...] = dot_nt(place_ref[...], local_ids.astype(BF16))
    lane = iota((owners, snaps), 1)
    ids = jnp.zeros((owners, snaps), F32)
    for k in range(SLOT):
        ids += jnp.where(lane == k, local_ref[pl.ds(k, owners, stride=SLOT), :], 0.0)
    out_ref[pl.ds(SLOT, owners, stride=WIDE), :] = ids
    for area in range(areas):
        block_copy(area).wait()
        right_copy(area).wait()
        chosen = dot(picks[area], block_ref[area]).astype(BF16)
        chosen_ref[area] = chosen
        solved = dot(chosen, right_ref[area * state : (area + 1) * state, :].astype(BF16))
        solved_ref[area * bound : (area + 1) * bound, :] = jnp.concatenate(split3(solved), axis=1)
    local_ref[...] = join3(dot(place_ref[...], solved_ref[...]), 0, snaps)
    for k in range(SLOT):
        at = pl.ds(k, owners, stride=SLOT)
        out_ref[pl.ds(k, owners, stride=WIDE), :] = local_ref[at, :]


def prepare_kernel(
    row_ref, var_ref, chosen_ref, rhs_ref,
    place_ref, mat_ref, term_ref, inner_ref,
    carry_ref, acc_ref,
):
    area = pl.program_id(0)
    slots = mat_ref.shape[0]
    state, snaps = rhs_ref.shape

    @pl.when(area == 0)
    def _():
        carry_ref[...] = jnp.zeros_like(carry_ref)
        acc_ref[...] = jnp.zeros_like(acc_ref)
        term_ref[...] = jnp.zeros_like(term_ref)

    row = row_ref[pl.ds(area, 1), :]
    var = var_ref[pl.ds(area, 1), :]
    place = placing(entry_slots(row, var, carry_ref, slots // SLOT), slots)
    place_ref[...] = place
    for at in range(0, state, BUILD):
        bound_rows = dot(placing(row - at, BUILD), jnp.ones((row.shape[1], snaps), BF16)) > 0.0
        inner_ref[at : at + BUILD, :] = jnp.where(
            bound_rows, 0.0, rhs_ref[at : at + BUILD, :]
        ).astype(BF16)
    at_rows = dot(picking(row, state), jnp.concatenate(split3(rhs_ref[...]), axis=1))
    coupling = dot(chosen_ref[0], placing(row, state))
    at_slots = dot(place, jnp.concatenate([at_rows, coupling], axis=1).astype(BF16))
    term_ref[...] += join3(at_slots, 0, snaps)
    acc_ref[...] += dot_nt(at_slots[:, 3 * snaps :].astype(BF16), place)

    @pl.when(area == pl.num_programs(0) - 1)
    def _():
        mat_ref[...] = acc_ref[...].astype(BF16)


def first_owner_kernel(in_ref, ret_ref, member_ref, inverse_ref):
    sources = in_ref.shape[0] // WIDE
    snaps = in_ref.shape[1]
    ids = in_ref[pl.ds(SLOT, sources, stride=WIDE), :].astype(jnp.int32)
    lane = iota((sources, 128), 1) + 1
    parts = [(ids[:, k : k + 1] == lane).astype(F32) for k in range(SLOT)]
    for k in range(SLOT):
        member_ref[pl.ds(k, sources, stride=SLOT), :] = parts[k]
    member = jnp.concatenate(parts, axis=0).astype(BF16)
    values = [in_ref[pl.ds(k, sources, stride=WIDE), :] for k in range(SLOT)]
    values = jnp.concatenate(values, axis=0)
    columns = jnp.concatenate(split3(values) + [jnp.ones(values.shape, BF16)], axis=1)
    sums = dot_t(member, columns)
    inverse = 1.0 / jnp.maximum(sums[:, 3 * snaps :], 1.0)
    inverse_ref[...] = inverse
    consensus = join3(sums, 0, snaps) * inverse
    back = join3(dot(member, jnp.concatenate(split3(consensus), axis=1)), 0, snaps)
    for k in range(SLOT):
        ret_ref[pl.ds(k, sources, stride=SLOT), :] = back[k * sources : (k + 1) * sources]


def states_kernel(
    row_ref, ginv_ref, inner_ref, place_ref, blend_ref, states_ref,
    block_ref, right_ref, solved_ref, block_sems, right_sems, out_sems,
):
    areas, bound = row_ref.shape
    state = ginv_ref.shape[1]

    def rows_of(area):
        return pl.ds(area * state, state)

    def right_copy(area):
        rows = rows_of(area)
        return pltpu.make_async_copy(inner_ref.at[rows], right_ref.at[rows], right_sems.at[area])

    def block_copy(area):
        return pltpu.make_async_copy(ginv_ref.at[area], block_ref.at[area], block_sems.at[area])

    def out_copy(area):
        rows = rows_of(area)
        return pltpu.make_async_copy(solved_ref.at[rows], states_ref.at[rows], out_sems.at[area])

    for area in range(areas):
        right_copy(area).start()
        block_copy(area).start()
    entry_rows = dot_t(place_ref[...], blend_ref[...]).astype(BF16)
    for area in range(areas):
        row = row_ref[area : area + 1, :]
        rows = entry_rows[area * bound : (area + 1) * bound]
        right_copy(area).wait()
        pieces = []
        for at in range(0, state, BUILD):
            placed = dot(placing(row - at, BUILD), rows).astype(BF16)
            pieces.append(right_ref[area * state + at : area * state + at + BUILD, :] + placed)
        blended = jnp.concatenate(pieces, axis=0)
        block_copy(area).wait()
        for at in range(0, state, PIECE):
            solved = dot(block_ref[area, at : at + PIECE, :], blended)
            solved_ref[area * state + at : area * state + at + PIECE, :] = solved
        out_copy(area).start()
    for area in range(areas):
        out_copy(area).wait()


def select(spec, a, b):
    return jnp.einsum(spec, a, b, precision=lax.Precision.HIGH, preferred_element_type=F32)


def shape(dims, dtype=F32):
    return jax.ShapeDtypeStruct(dims, dtype)


def on_device(ginv, rhs, bnd_row, bnd_var):
    areas, state, _ = ginv.shape
    snaps = rhs.shape[1]
    bound = bnd_row.shape[1]
    devices = lax.axis_size("area") * lax.axis_size("tie")
    slots = devices * SLOT
    entries = areas * bound

    def whole(*dims):
        return pl.BlockSpec(dims, lambda a: (0,) * len(dims))

    in_order = pltpu.CompilerParams(dimension_semantics=("arbitrary",))
    anywhere = pl.BlockSpec(memory_space=pl.ANY)
    small = pl.BlockSpec((areas, bound), lambda: (0, 0))
    local, outgoing, chosen = pl.pallas_call(
        start_kernel,
        in_specs=[small, small, anywhere, anywhere],
        out_shape=[
            pltpu.VMEM((slots, snaps), F32),
            pltpu.VMEM((devices * WIDE, snaps), F32),
            pltpu.VMEM((areas, bound, state), BF16),
        ],
        scratch_shapes=[
            pltpu.VMEM((areas, state, state), BF16),
            pltpu.VMEM((areas * state, snaps), F32),
            pltpu.VMEM((devices, bound), F32),
            pltpu.VMEM((slots, entries), BF16),
            pltpu.VMEM((entries, 3 * snaps), BF16),
            pltpu.SemaphoreType.DMA((areas,)),
            pltpu.SemaphoreType.DMA((areas,)),
        ],
        name="start",
    )(bnd_row, bnd_var, ginv, rhs)
    place, mat, term, inner = pl.pallas_call(
        prepare_kernel,
        grid=(areas,),
        in_specs=[
            whole(areas, bound),
            whole(areas, bound),
            pl.BlockSpec((1, bound, state), lambda a: (a, 0, 0)),
            pl.BlockSpec((state, snaps), lambda a: (a, 0)),
        ],
        out_specs=[
            pl.BlockSpec((slots, bound), lambda a: (0, a)),
            whole(slots, slots),
            whole(slots, snaps),
            pl.BlockSpec((state, snaps), lambda a: (a, 0)),
        ],
        out_shape=[
            pltpu.VMEM((slots, entries), BF16),
            pltpu.VMEM((slots, slots), BF16),
            pltpu.VMEM((slots, snaps), F32),
            shape((areas * state, snaps), BF16),
        ],
        scratch_shapes=[pltpu.VMEM((devices, bound), F32), pltpu.VMEM((slots, slots), F32)],
        compiler_params=in_order,
        name="prepare",
    )(bnd_row, bnd_var, chosen, rhs)

    def exchange(x, rows=SLOT, width=snaps):
        x = x.reshape(devices, rows, width)
        x = lax.all_to_all(x, ("area", "tie"), split_axis=0, concat_axis=0, tiled=True)
        return x.reshape(-1, snaps)

    base = local - dot(mat, term.astype(BF16))
    received, place, mat, base, term, inner = lax.optimization_barrier(
        (exchange(outgoing, 1, WIDE * snaps), place, mat, base, term, inner)
    )
    returning, member, inverse = pl.pallas_call(
        first_owner_kernel,
        in_specs=[pl.BlockSpec(memory_space=pltpu.VMEM)],
        out_shape=[
            pltpu.VMEM((slots, snaps), F32),
            pltpu.VMEM((slots, 128), F32),
            pltpu.VMEM((128, snaps), F32),
        ],
        name="first_owner",
    )(pltpu.with_memory_space_constraint(received, pltpu.VMEM))
    for iteration in range(ITERS):
        if iteration > 0:
            blend = (term + PENALTY * (agreed - dual)).astype(BF16)
            local = (base + dot(mat, blend)) + dual
            consensus = select("sv,sn->vn", member, exchange(local)) * inverse
            returning = select("sv,vn->sn", member, consensus)
        agreed = exchange(returning)
        dual = local - agreed
    consensus = consensus[:VAR_DEV]
    states = pl.pallas_call(
        states_kernel,
        in_specs=[
            small,
            anywhere,
            anywhere,
            pl.BlockSpec((slots, entries), lambda: (0, 0)),
            pl.BlockSpec((slots, snaps), lambda: (0, 0)),
        ],
        out_specs=anywhere,
        out_shape=shape((areas * state, snaps)),
        scratch_shapes=[
            pltpu.VMEM((areas, state, state), BF16),
            pltpu.VMEM((areas * state, snaps), BF16),
            pltpu.VMEM((areas * state, snaps), F32),
            pltpu.SemaphoreType.DMA((areas,)),
            pltpu.SemaphoreType.DMA((areas,)),
            pltpu.SemaphoreType.DMA((areas,)),
        ],
        name="states",
    )(bnd_row, ginv, inner, place, blend)
    dual = select("se,sn->en", place.astype(F32), dual)
    return states, consensus, dual


def solution(mesh):
    both = ("area", "tie")
    return jax.shard_map(
        on_device,
        mesh=mesh,
        in_specs=(P(both, None, None), P(both, None), P(both, None), P(both, None)),
        out_specs=(P(both, None), P(both, None), P(both, None)),
        check_vma=False,
    )
```

```python
import jax
import jax.numpy as jnp
from jax import lax
from jax.experimental import pallas as pl
from jax.experimental.pallas import tpu as pltpu
from jax.sharding import PartitionSpec as P

SLOT = 4
VAR_DEV = 64
ITERS = 4
PENALTY = 1.0
PIECE = 128
BUILD = 256
WIDE = SLOT + 1

F32 = jnp.float32
BF16 = jnp.bfloat16


def split3(x):
    hi = x.astype(BF16)
    rest = x - hi.astype(F32)
    mid = rest.astype(BF16)
    low = (rest - mid.astype(F32)).astype(BF16)
    return [hi, mid, low]


def join3(y, at=0, width=128):
    return (y[:, at : at + width] + y[:, at + width : at + 2 * width]) + y[
        :, at + 2 * width : at + 3 * width
    ]


def dot(a, b):
    return jnp.dot(a, b, preferred_element_type=F32)


def dot_t(a, b):
    return lax.dot_general(a, b, (((0,), (0,)), ((), ())), preferred_element_type=F32)


def iota(shape, dim):
    return lax.broadcasted_iota(jnp.int32, shape, dim)


def entry_slots(row, var, carry_ref, owners):
    bound = row.shape[1]
    live = row >= 0
    owner = jnp.where(live, lax.shift_right_arithmetic(var, 6), -1)
    owned = iota((owners, bound), 0) == owner
    owned_f = owned.astype(F32)
    before = (iota((bound, bound), 0) < iota((bound, bound), 1)).astype(F32).astype(BF16)
    earlier = dot(owned_f.astype(BF16), before)
    rank = jnp.sum(jnp.where(owned, earlier + carry_ref[...], 0.0), axis=0, keepdims=True)
    carry_ref[...] += jnp.sum(owned_f, axis=1, keepdims=True)
    return jnp.where(live, owner * SLOT + rank.astype(jnp.int32), -1)


def placing(slot, slots):
    return (iota((slots, slot.shape[1]), 0) == slot).astype(F32).astype(BF16)


def picking(row, state):
    bound = row.shape[1]
    down = jnp.broadcast_to(row.astype(F32), (bound, bound)).T.astype(jnp.int32)
    lane = iota((bound, bound), 1)
    parts = [(lane + at == down).astype(F32) for at in range(0, state, bound)]
    return jnp.concatenate(parts, axis=1).astype(BF16)


def start_kernel(
    row_ref, var_ref, ginv_ref, rhs_ref, local_ref, out_ref, chosen_ref,
    block_ref, right_ref, picked_ref, carry_ref, place_ref, solved_ref,
    block_sems, right_sems, out_sems,
):
    areas, bound = row_ref.shape
    state = ginv_ref.shape[1]
    slots, snaps = local_ref.shape
    owners = slots // SLOT

    def block_copy(area):
        return pltpu.make_async_copy(ginv_ref.at[area], block_ref.at[area], block_sems.at[area])

    def right_copy(area):
        rows = pl.ds(area * state, state)
        return pltpu.make_async_copy(rhs_ref.at[rows], right_ref.at[rows], right_sems.at[area])

    def out_copy(area):
        return pltpu.make_async_copy(picked_ref.at[area], chosen_ref.at[area], out_sems.at[area])

    for area in range(areas):
        block_copy(area).start()
        right_copy(area).start()
    carry_ref[...] = jnp.zeros_like(carry_ref)
    picks = []
    local_ids = []
    for area in range(areas):
        row = row_ref[area : area + 1, :]
        var = var_ref[area : area + 1, :]
        place_ref[:, area * bound : (area + 1) * bound] = placing(
            entry_slots(row, var, carry_ref, owners), slots
        )
        picks.append(picking(row, state))
        local_id = jnp.where(row >= 0, (var & (VAR_DEV - 1)) + 1, 0).astype(F32)
        local_ids.append(jnp.broadcast_to(local_id, (snaps, bound)).T.astype(BF16))
    local_ids = jnp.concatenate(local_ids, axis=0)
    for at in range(0, slots, PIECE):
        local_ref[at : at + PIECE, :] = dot(place_ref[at : at + PIECE, :], local_ids)
    lane = iota((owners, snaps), 1)
    ids = jnp.zeros((owners, snaps), F32)
    for k in range(SLOT):
        ids += jnp.where(lane == k, local_ref[pl.ds(k, owners, stride=SLOT), :], 0.0)
    out_ref[pl.ds(SLOT, owners, stride=WIDE), :] = ids
    for area in range(areas):
        block_copy(area).wait()
        right_copy(area).wait()
        for at in range(0, state, BUILD):
            part = dot(picks[area], block_ref[area, :, at : at + BUILD])
            picked_ref[area, :, at : at + BUILD] = part.astype(BF16)
        out_copy(area).start()
        right = right_ref[area * state : (area + 1) * state, :].astype(BF16)
        solved = dot(picked_ref[area], right)
        solved_ref[area * bound : (area + 1) * bound, :] = jnp.concatenate(split3(solved), axis=1)
    for at in range(0, slots, PIECE):
        local_ref[at : at + PIECE, :] = join3(dot(place_ref[at : at + PIECE, :], solved_ref[...]), 0, snaps)
    for k in range(SLOT):
        at = pl.ds(k, owners, stride=SLOT)
        out_ref[pl.ds(k, owners, stride=WIDE), :] = local_ref[at, :]
    for area in range(areas):
        out_copy(area).wait()


def prepare_kernel(
    row_ref, var_ref, chosen_ref, rhs_ref, back_ref, mat_ref, term_ref, inner_ref,
    picked_ref, right_ref, kept_ref, carry_ref, rows_ref, spread_ref, place_ref,
    picked_sems, right_sems, out_sems,
):
    areas, bound = row_ref.shape
    state = chosen_ref.shape[2]
    slots, snaps = term_ref.shape

    def picked_copy(area):
        return pltpu.make_async_copy(chosen_ref.at[area], picked_ref.at[area], picked_sems.at[area])

    def right_copy(area):
        rows = pl.ds(area * state, state)
        return pltpu.make_async_copy(rhs_ref.at[rows], right_ref.at[rows], right_sems.at[area])

    def out_copy(area):
        rows = pl.ds(area * state, state)
        return pltpu.make_async_copy(kept_ref.at[rows], inner_ref.at[rows], out_sems.at[area])

    for area in range(areas):
        right_copy(area).start()
        picked_copy(area).start()
    carry_ref[...] = jnp.zeros_like(carry_ref)
    for area in range(areas):
        var = var_ref[area : area + 1, :]
        slot = entry_slots(row_ref[area : area + 1, :], var, carry_ref, slots // SLOT)
        entries = slice(area * bound, (area + 1) * bound)
        place_ref[:, entries] = placing(slot, slots)
        back_ref[entries, :] = picking(slot, slots)
    ones = jnp.ones((bound, snaps), BF16)
    for area in range(areas):
        entries = slice(area * bound, (area + 1) * bound)
        row = row_ref[area : area + 1, :]
        right_copy(area).wait()
        for at in range(0, state, BUILD):
            here = slice(area * state + at, area * state + at + BUILD)
            is_bound = dot(placing(row - at, BUILD), ones) > 0.0
            kept_ref[here, :] = jnp.where(is_bound, 0.0, right_ref[here, :]).astype(BF16)
        out_copy(area).start()
        right = right_ref[area * state : (area + 1) * state, :]
        at_rows = dot(picking(row, state), jnp.concatenate(split3(right), axis=1))
        rows_ref[entries, :] = at_rows.astype(BF16)
        picked_copy(area).wait()
        coupling = dot(picked_ref[area], placing(row, state)).astype(BF16)
        for at in range(0, slots, PIECE):
            spread = dot(place_ref[at : at + PIECE, entries], coupling)
            spread_ref[at : at + PIECE, entries] = spread.astype(BF16)
    for at in range(0, slots, PIECE):
        here = slice(at, at + PIECE)
        term_ref[here, :] = join3(dot(place_ref[here, :], rows_ref[...]), 0, snaps)
        mat_ref[here, :] = dot(spread_ref[here, :], back_ref[...]).astype(BF16)
    for area in range(areas):
        out_copy(area).wait()


def first_owner_kernel(in_ref, ret_ref, member_ref, inverse_ref):
    sources = in_ref.shape[0] // WIDE
    snaps = in_ref.shape[1]
    ids = in_ref[pl.ds(SLOT, sources, stride=WIDE), :].astype(jnp.int32)
    lane = iota((sources, 128), 1) + 1
    parts = [(ids[:, k : k + 1] == lane).astype(F32) for k in range(SLOT)]
    for k in range(SLOT):
        member_ref[pl.ds(k, sources, stride=SLOT), :] = parts[k][:, :VAR_DEV]
    member = jnp.concatenate(parts, axis=0).astype(BF16)
    values = [in_ref[pl.ds(k, sources, stride=WIDE), :] for k in range(SLOT)]
    values = jnp.concatenate(values, axis=0)
    columns = jnp.concatenate(split3(values) + [jnp.ones(values.shape, BF16)], axis=1)
    sums = dot_t(member, columns)
    inverse = 1.0 / jnp.maximum(sums[:, 3 * snaps :], 1.0)
    inverse_ref[...] = inverse[:VAR_DEV]
    consensus = join3(sums, 0, snaps) * inverse
    back = join3(dot(member, jnp.concatenate(split3(consensus), axis=1)), 0, snaps)
    for k in range(SLOT):
        ret_ref[pl.ds(k, sources, stride=SLOT), :] = back[k * sources : (k + 1) * sources]


def states_kernel(
    row_ref, ginv_ref, inner_ref, back_ref, blend_ref, states_ref,
    block_ref, right_ref, solved_ref, block_sems, right_sems, out_sems,
):
    areas, bound = row_ref.shape
    state = ginv_ref.shape[1]

    def rows_of(area):
        return pl.ds(area * state, state)

    def right_copy(area):
        rows = rows_of(area)
        return pltpu.make_async_copy(inner_ref.at[rows], right_ref.at[rows], right_sems.at[area])

    def block_copy(area):
        return pltpu.make_async_copy(ginv_ref.at[area], block_ref.at[area], block_sems.at[area])

    def out_copy(area):
        rows = rows_of(area)
        return pltpu.make_async_copy(solved_ref.at[rows], states_ref.at[rows], out_sems.at[area])

    for area in range(areas):
        right_copy(area).start()
        block_copy(area).start()
    entry_rows = dot(back_ref[...], blend_ref[...]).astype(BF16)
    for area in range(areas):
        row = row_ref[area : area + 1, :]
        rows = entry_rows[area * bound : (area + 1) * bound]
        right_copy(area).wait()
        pieces = []
        for at in range(0, state, BUILD):
            placed = dot(placing(row - at, BUILD), rows).astype(BF16)
            pieces.append(right_ref[area * state + at : area * state + at + BUILD, :] + placed)
        blended = jnp.concatenate(pieces, axis=0)
        block_copy(area).wait()
        for at in range(0, state, PIECE):
            solved = dot(block_ref[area, at : at + PIECE, :], blended)
            solved_ref[area * state + at : area * state + at + PIECE, :] = solved
        out_copy(area).start()
    for area in range(areas):
        out_copy(area).wait()


def select(spec, a, b):
    return jnp.einsum(spec, a, b, precision=lax.Precision.HIGH, preferred_element_type=F32)


def shape(dims, dtype=F32):
    return jax.ShapeDtypeStruct(dims, dtype)


def on_device(ginv, rhs, bnd_row, bnd_var):
    areas, state, _ = ginv.shape
    snaps = rhs.shape[1]
    bound = bnd_row.shape[1]
    devices = lax.axis_size("area") * lax.axis_size("tie")
    slots = devices * SLOT
    entries = areas * bound

    anywhere = pl.BlockSpec(memory_space=pl.ANY)
    small = pl.BlockSpec((areas, bound), lambda: (0, 0))
    whole = pl.BlockSpec(memory_space=pltpu.VMEM)
    local, outgoing, chosen = pl.pallas_call(
        start_kernel,
        in_specs=[small, small, anywhere, anywhere],
        out_specs=[whole, whole, anywhere],
        out_shape=[
            pltpu.VMEM((slots, snaps), F32),
            pltpu.VMEM((devices * WIDE, snaps), F32),
            shape((areas, bound, state), BF16),
        ],
        scratch_shapes=[
            pltpu.VMEM((areas, state, state), BF16),
            pltpu.VMEM((areas * state, snaps), F32),
            pltpu.VMEM((areas, bound, state), BF16),
            pltpu.VMEM((devices, bound), F32),
            pltpu.VMEM((slots, entries), BF16),
            pltpu.VMEM((entries, 3 * snaps), BF16),
            pltpu.SemaphoreType.DMA((areas,)),
            pltpu.SemaphoreType.DMA((areas,)),
            pltpu.SemaphoreType.DMA((areas,)),
        ],
        name="start",
    )(bnd_row, bnd_var, ginv, rhs)
    back, mat, term, inner = pl.pallas_call(
        prepare_kernel,
        in_specs=[small, small, anywhere, anywhere],
        out_specs=[whole, whole, whole, anywhere],
        out_shape=[
            pltpu.VMEM((entries, slots), BF16),
            pltpu.VMEM((slots, slots), BF16),
            pltpu.VMEM((slots, snaps), F32),
            shape((areas * state, snaps), BF16),
        ],
        scratch_shapes=[
            pltpu.VMEM((areas, bound, state), BF16),
            pltpu.VMEM((areas * state, snaps), F32),
            pltpu.VMEM((areas * state, snaps), BF16),
            pltpu.VMEM((devices, bound), F32),
            pltpu.VMEM((entries, 3 * snaps), BF16),
            pltpu.VMEM((slots, entries), BF16),
            pltpu.VMEM((slots, entries), BF16),
            pltpu.SemaphoreType.DMA((areas,)),
            pltpu.SemaphoreType.DMA((areas,)),
            pltpu.SemaphoreType.DMA((areas,)),
        ],
        name="prepare",
    )(bnd_row, bnd_var, chosen, rhs)

    def exchange(x, rows=SLOT, width=snaps):
        x = x.reshape(devices, rows, width)
        x = lax.all_to_all(x, ("area", "tie"), split_axis=0, concat_axis=0, tiled=True)
        return x.reshape(-1, snaps)

    base = local - dot(mat, term.astype(BF16))
    received, back, mat, base, term, inner = lax.optimization_barrier(
        (exchange(outgoing, 1, WIDE * snaps), back, mat, base, term, inner)
    )
    returning, member, inverse = pl.pallas_call(
        first_owner_kernel,
        in_specs=[whole],
        out_shape=[
            pltpu.VMEM((slots, snaps), F32),
            pltpu.VMEM((slots, VAR_DEV), F32),
            pltpu.VMEM((VAR_DEV, snaps), F32),
        ],
        name="first_owner",
    )(pltpu.with_memory_space_constraint(received, pltpu.VMEM))
    for iteration in range(ITERS):
        if iteration > 0:
            blend = (term + PENALTY * (agreed - dual)).astype(BF16)
            local = (base + dot(mat, blend)) + dual
            consensus = select("sv,sn->vn", member, exchange(local)) * inverse
            returning = select("sv,vn->sn", member, consensus)
        agreed = exchange(returning)
        dual = local - agreed
    states = pl.pallas_call(
        states_kernel,
        in_specs=[
            small,
            anywhere,
            anywhere,
            pl.BlockSpec((entries, slots), lambda: (0, 0)),
            pl.BlockSpec((slots, snaps), lambda: (0, 0)),
        ],
        out_specs=anywhere,
        out_shape=shape((areas * state, snaps)),
        scratch_shapes=[
            pltpu.VMEM((areas, state, state), BF16),
            pltpu.VMEM((areas * state, snaps), BF16),
            pltpu.VMEM((areas * state, snaps), F32),
            pltpu.SemaphoreType.DMA((areas,)),
            pltpu.SemaphoreType.DMA((areas,)),
            pltpu.SemaphoreType.DMA((areas,)),
        ],
        name="states",
    )(bnd_row, ginv, inner, back, blend)
    dual = select("es,sn->en", back.astype(F32), dual)
    return states, consensus, dual


def solution(mesh):
    both = ("area", "tie")
    return jax.shard_map(
        on_device,
        mesh=mesh,
        in_specs=(P(both, None, None), P(both, None), P(both, None), P(both, None)),
        out_specs=(P(both, None), P(both, None), P(both, None)),
        check_vma=False,
    )
```

```python
import jax
import jax.numpy as jnp
from jax import lax
from jax.experimental import pallas as pl
from jax.experimental.pallas import tpu as pltpu
from jax.sharding import PartitionSpec as P

SLOT = 4
VAR_DEV = 64
ITERS = 4
PENALTY = 1.0
PIECE = 128
BUILD = 256
OUT = 512
WIDE = SLOT + 1

F32 = jnp.float32
BF16 = jnp.bfloat16


def split3(x):
    hi = x.astype(BF16)
    rest = x - hi.astype(F32)
    mid = rest.astype(BF16)
    low = (rest - mid.astype(F32)).astype(BF16)
    return [hi, mid, low]


def join3(y, at=0, width=128):
    return (y[:, at : at + width] + y[:, at + width : at + 2 * width]) + y[
        :, at + 2 * width : at + 3 * width
    ]


def dot(a, b):
    return jnp.dot(a, b, preferred_element_type=F32)


def dot_t(a, b):
    return lax.dot_general(a, b, (((0,), (0,)), ((), ())), preferred_element_type=F32)


def iota(shape, dim):
    return lax.broadcasted_iota(jnp.int32, shape, dim)


def entry_slots(row, var, carry_ref, owners):
    bound = row.shape[1]
    live = row >= 0
    owner = jnp.where(live, lax.shift_right_arithmetic(var, 6), -1)
    owned = iota((owners, bound), 0) == owner
    owned_f = owned.astype(F32)
    before = (iota((bound, bound), 0) < iota((bound, bound), 1)).astype(F32).astype(BF16)
    earlier = dot(owned_f.astype(BF16), before)
    rank = jnp.sum(jnp.where(owned, earlier + carry_ref[...], 0.0), axis=0, keepdims=True)
    carry_ref[...] += jnp.sum(owned_f, axis=1, keepdims=True)
    return jnp.where(live, owner * SLOT + rank.astype(jnp.int32), -1)


def placing(slot, slots):
    return (iota((slots, slot.shape[1]), 0) == slot).astype(F32).astype(BF16)


def picking(row, state):
    bound = row.shape[1]
    down = jnp.broadcast_to(row.astype(F32), (bound, bound)).T.astype(jnp.int32)
    lane = iota((bound, bound), 1)
    parts = [(lane + at == down).astype(F32) for at in range(0, state, bound)]
    return jnp.concatenate(parts, axis=1).astype(BF16)


def start_kernel(
    row_ref, var_ref, ginv_ref, rhs_ref, local_ref, out_ref, couple_ref,
    block_ref, right_ref, picked_ref, carry_ref, place_ref, solved_ref,
    block_sems, right_sems,
):
    areas, bound = row_ref.shape
    state = ginv_ref.shape[1]
    slots, snaps = local_ref.shape
    owners = slots // SLOT

    def block_copy(area):
        return pltpu.make_async_copy(ginv_ref.at[area], block_ref.at[area], block_sems.at[area])

    def right_copy(area):
        rows = pl.ds(area * state, state)
        return pltpu.make_async_copy(rhs_ref.at[rows], right_ref.at[rows], right_sems.at[area])

    for area in range(areas):
        block_copy(area).start()
        right_copy(area).start()
    carry_ref[...] = jnp.zeros_like(carry_ref)
    picks = []
    columns = []
    local_ids = []
    for area in range(areas):
        row = row_ref[area : area + 1, :]
        var = var_ref[area : area + 1, :]
        place_ref[:, area * bound : (area + 1) * bound] = placing(
            entry_slots(row, var, carry_ref, owners), slots
        )
        picks.append(picking(row, state))
        columns.append(placing(row, state))
        local_id = jnp.where(row >= 0, (var & (VAR_DEV - 1)) + 1, 0).astype(F32)
        local_ids.append(jnp.broadcast_to(local_id, (snaps, bound)).T.astype(BF16))
    local_ids = jnp.concatenate(local_ids, axis=0)
    for at in range(0, slots, PIECE):
        local_ref[at : at + PIECE, :] = dot(place_ref[at : at + PIECE, :], local_ids)
    lane = iota((owners, snaps), 1)
    ids = jnp.zeros((owners, snaps), F32)
    for k in range(SLOT):
        ids += jnp.where(lane == k, local_ref[pl.ds(k, owners, stride=SLOT), :], 0.0)
    out_ref[pl.ds(SLOT, owners, stride=WIDE), :] = ids
    for area in range(areas):
        block_copy(area).wait()
        right_copy(area).wait()
        for at in range(0, state, BUILD):
            part = dot(picks[area], block_ref[area, :, at : at + BUILD])
            picked_ref[:, at : at + BUILD] = part.astype(BF16)
        right = right_ref[area * state : (area + 1) * state, :].astype(BF16)
        both = dot(picked_ref[...], jnp.concatenate([right, columns[area]], axis=1))
        solved = both[:, :snaps]
        couple_ref[area] = both[:, snaps:].astype(BF16)
        solved_ref[area * bound : (area + 1) * bound, :] = jnp.concatenate(split3(solved), axis=1)
    for at in range(0, slots, PIECE):
        local_ref[at : at + PIECE, :] = join3(dot(place_ref[at : at + PIECE, :], solved_ref[...]), 0, snaps)
    for k in range(SLOT):
        at = pl.ds(k, owners, stride=SLOT)
        out_ref[pl.ds(k, owners, stride=WIDE), :] = local_ref[at, :]


def prepare_kernel(
    row_ref, var_ref, couple_ref, rhs_ref, back_ref, mat_ref, term_ref, inner_ref,
    right_ref, kept_ref, carry_ref, rows_ref, spread_ref, place_ref,
    right_sems, out_sems,
):
    areas, bound = row_ref.shape
    state = rhs_ref.shape[0] // areas
    slots, snaps = term_ref.shape

    def right_copy(area):
        rows = pl.ds(area * state, state)
        return pltpu.make_async_copy(rhs_ref.at[rows], right_ref.at[rows], right_sems.at[area])

    def out_copy(area):
        rows = pl.ds(area * state, state)
        return pltpu.make_async_copy(kept_ref.at[rows], inner_ref.at[rows], out_sems.at[area])

    for area in range(areas):
        right_copy(area).start()
    carry_ref[...] = jnp.zeros_like(carry_ref)
    for area in range(areas):
        var = var_ref[area : area + 1, :]
        slot = entry_slots(row_ref[area : area + 1, :], var, carry_ref, slots // SLOT)
        entries = slice(area * bound, (area + 1) * bound)
        place_ref[:, entries] = placing(slot, slots)
        back_ref[entries, :] = picking(slot, slots)
    ones = jnp.ones((bound, snaps), BF16)
    for area in range(areas):
        entries = slice(area * bound, (area + 1) * bound)
        row = row_ref[area : area + 1, :]
        right_copy(area).wait()
        for at in range(0, state, BUILD):
            here = slice(area * state + at, area * state + at + BUILD)
            is_bound = dot(placing(row - at, BUILD), ones) > 0.0
            kept_ref[here, :] = jnp.where(is_bound, 0.0, right_ref[here, :]).astype(BF16)
        out_copy(area).start()
        right = right_ref[area * state : (area + 1) * state, :]
        at_rows = dot(picking(row, state), jnp.concatenate(split3(right), axis=1))
        rows_ref[entries, :] = at_rows.astype(BF16)
        for at in range(0, slots, PIECE):
            spread = dot(place_ref[at : at + PIECE, entries], couple_ref[area])
            spread_ref[at : at + PIECE, entries] = spread.astype(BF16)
    for at in range(0, slots, PIECE):
        here = slice(at, at + PIECE)
        term_ref[here, :] = join3(dot(place_ref[here, :], rows_ref[...]), 0, snaps)
        mat_ref[here, :] = dot(spread_ref[here, :], back_ref[...]).astype(BF16)
    for area in range(areas):
        out_copy(area).wait()


def first_owner_kernel(in_ref, ret_ref, member_ref, inverse_ref):
    sources = in_ref.shape[0] // WIDE
    snaps = in_ref.shape[1]
    ids = in_ref[pl.ds(SLOT, sources, stride=WIDE), :].astype(jnp.int32)
    lane = iota((sources, 128), 1) + 1
    parts = [(ids[:, k : k + 1] == lane).astype(F32) for k in range(SLOT)]
    for k in range(SLOT):
        member_ref[pl.ds(k, sources, stride=SLOT), :] = parts[k][:, :VAR_DEV]
    member = jnp.concatenate(parts, axis=0).astype(BF16)
    values = [in_ref[pl.ds(k, sources, stride=WIDE), :] for k in range(SLOT)]
    values = jnp.concatenate(values, axis=0)
    columns = jnp.concatenate(split3(values) + [jnp.ones(values.shape, BF16)], axis=1)
    sums = dot_t(member, columns)
    inverse = 1.0 / jnp.maximum(sums[:, 3 * snaps :], 1.0)
    inverse_ref[...] = inverse[:VAR_DEV]
    consensus = join3(sums, 0, snaps) * inverse
    back = join3(dot(member, jnp.concatenate(split3(consensus), axis=1)), 0, snaps)
    for k in range(SLOT):
        ret_ref[pl.ds(k, sources, stride=SLOT), :] = back[k * sources : (k + 1) * sources]


def states_kernel(
    row_ref, ginv_ref, inner_ref, back_ref, blend_ref, states_ref,
    block_ref, right_ref, solved_ref, block_sems, right_sems, out_sems,
):
    areas, bound = row_ref.shape
    state = ginv_ref.shape[1]

    def rows_of(area):
        return pl.ds(area * state, state)

    def right_copy(area):
        rows = rows_of(area)
        return pltpu.make_async_copy(inner_ref.at[rows], right_ref.at[rows], right_sems.at[area])

    def block_copy(area):
        return pltpu.make_async_copy(ginv_ref.at[area], block_ref.at[area], block_sems.at[area])

    def out_copy(piece):
        rows = pl.ds(piece * OUT, OUT)
        return pltpu.make_async_copy(solved_ref.at[rows], states_ref.at[rows], out_sems.at[piece])

    for area in range(areas):
        right_copy(area).start()
        block_copy(area).start()
    entry_rows = dot(back_ref[...], blend_ref[...]).astype(BF16)
    for area in range(areas):
        row = row_ref[area : area + 1, :]
        rows = entry_rows[area * bound : (area + 1) * bound]
        right_copy(area).wait()
        pieces = []
        for at in range(0, state, BUILD):
            placed = dot(placing(row - at, BUILD), rows).astype(BF16)
            pieces.append(right_ref[area * state + at : area * state + at + BUILD, :] + placed)
        blended = jnp.concatenate(pieces, axis=0)
        block_copy(area).wait()
        for at in range(0, state, PIECE):
            solved = dot(block_ref[area, at : at + PIECE, :], blended)
            solved_ref[area * state + at : area * state + at + PIECE, :] = solved
            if (at + PIECE) % OUT == 0:
                out_copy((area * state + at) // OUT).start()
    for piece in range(areas * state // OUT):
        out_copy(piece).wait()


def select(spec, a, b):
    return jnp.einsum(spec, a, b, precision=lax.Precision.HIGH, preferred_element_type=F32)


def shape(dims, dtype=F32):
    return jax.ShapeDtypeStruct(dims, dtype)


def on_device(ginv, rhs, bnd_row, bnd_var):
    areas, state, _ = ginv.shape
    snaps = rhs.shape[1]
    bound = bnd_row.shape[1]
    devices = lax.axis_size("area") * lax.axis_size("tie")
    slots = devices * SLOT
    entries = areas * bound

    anywhere = pl.BlockSpec(memory_space=pl.ANY)
    small = pl.BlockSpec((areas, bound), lambda: (0, 0))
    whole = pl.BlockSpec(memory_space=pltpu.VMEM)
    local, outgoing, couple = pl.pallas_call(
        start_kernel,
        in_specs=[small, small, anywhere, anywhere],
        out_specs=[whole, whole, whole],
        out_shape=[
            pltpu.VMEM((slots, snaps), F32),
            pltpu.VMEM((devices * WIDE, snaps), F32),
            shape((areas, bound, bound), BF16),
        ],
        scratch_shapes=[
            pltpu.VMEM((areas, state, state), BF16),
            pltpu.VMEM((areas * state, snaps), F32),
            pltpu.VMEM((bound, state), BF16),
            pltpu.VMEM((devices, bound), F32),
            pltpu.VMEM((slots, entries), BF16),
            pltpu.VMEM((entries, 3 * snaps), BF16),
            pltpu.SemaphoreType.DMA((areas,)),
            pltpu.SemaphoreType.DMA((areas,)),
        ],
        name="start",
    )(bnd_row, bnd_var, ginv, rhs)
    back, mat, term, inner = pl.pallas_call(
        prepare_kernel,
        in_specs=[small, small, whole, anywhere],
        out_specs=[whole, whole, whole, anywhere],
        out_shape=[
            pltpu.VMEM((entries, slots), BF16),
            pltpu.VMEM((slots, slots), BF16),
            pltpu.VMEM((slots, snaps), F32),
            shape((areas * state, snaps), BF16),
        ],
        scratch_shapes=[
            pltpu.VMEM((areas * state, snaps), F32),
            pltpu.VMEM((areas * state, snaps), BF16),
            pltpu.VMEM((devices, bound), F32),
            pltpu.VMEM((entries, 3 * snaps), BF16),
            pltpu.VMEM((slots, entries), BF16),
            pltpu.VMEM((slots, entries), BF16),
            pltpu.SemaphoreType.DMA((areas,)),
            pltpu.SemaphoreType.DMA((areas,)),
        ],
        name="prepare",
    )(bnd_row, bnd_var, couple, rhs)

    def exchange(x, rows=SLOT, width=snaps):
        x = x.reshape(devices, rows, width)
        x = lax.all_to_all(x, ("area", "tie"), split_axis=0, concat_axis=0, tiled=True)
        return x.reshape(-1, snaps)

    base = local - dot(mat, term.astype(BF16))
    received, back, mat, base, term, inner = lax.optimization_barrier(
        (exchange(outgoing, 1, WIDE * snaps), back, mat, base, term, inner)
    )
    returning, member, inverse = pl.pallas_call(
        first_owner_kernel,
        in_specs=[whole],
        out_shape=[
            pltpu.VMEM((slots, snaps), F32),
            pltpu.VMEM((slots, VAR_DEV), F32),
            pltpu.VMEM((VAR_DEV, snaps), F32),
        ],
        name="first_owner",
    )(pltpu.with_memory_space_constraint(received, pltpu.VMEM))
    for iteration in range(ITERS):
        if iteration > 0:
            blend = (term + PENALTY * (agreed - dual)).astype(BF16)
            local = (base + dot(mat, blend)) + dual
            consensus = select("sv,sn->vn", member, exchange(local)) * inverse
            returning = select("sv,vn->sn", member, consensus)
        agreed = exchange(returning)
        dual = local - agreed
    states = pl.pallas_call(
        states_kernel,
        in_specs=[
            small,
            anywhere,
            anywhere,
            pl.BlockSpec((entries, slots), lambda: (0, 0)),
            pl.BlockSpec((slots, snaps), lambda: (0, 0)),
        ],
        out_specs=anywhere,
        out_shape=shape((areas * state, snaps)),
        scratch_shapes=[
            pltpu.VMEM((areas, state, state), BF16),
            pltpu.VMEM((areas * state, snaps), BF16),
            pltpu.VMEM((areas * state, snaps), F32),
            pltpu.SemaphoreType.DMA((areas,)),
            pltpu.SemaphoreType.DMA((areas,)),
            pltpu.SemaphoreType.DMA((areas * state // OUT,)),
        ],
        name="states",
    )(bnd_row, ginv, inner, back, blend)
    dual = select("es,sn->en", back.astype(F32), dual)
    return states, consensus, dual


def solution(mesh):
    both = ("area", "tie")
    return jax.shard_map(
        on_device,
        mesh=mesh,
        in_specs=(P(both, None, None), P(both, None), P(both, None), P(both, None)),
        out_specs=(P(both, None), P(both, None), P(both, None)),
        check_vma=False,
    )
```

```python
import jax
import jax.numpy as jnp
from jax import lax
from jax.experimental import pallas as pl
from jax.experimental.pallas import tpu as pltpu
from jax.sharding import PartitionSpec as P

SLOT = 4
VAR_DEV = 64
ITERS = 4
PENALTY = 1.0
PIECE = 128
BUILD = 256
OUT = 512
WIDE = SLOT + 1

F32 = jnp.float32
BF16 = jnp.bfloat16


def split3(x):
    hi = x.astype(BF16)
    rest = x - hi.astype(F32)
    mid = rest.astype(BF16)
    low = (rest - mid.astype(F32)).astype(BF16)
    return [hi, mid, low]


def join3(y, at=0, width=128):
    return (y[:, at : at + width] + y[:, at + width : at + 2 * width]) + y[
        :, at + 2 * width : at + 3 * width
    ]


def dot(a, b):
    return jnp.dot(a, b, preferred_element_type=F32)


def dot_t(a, b):
    return lax.dot_general(a, b, (((0,), (0,)), ((), ())), preferred_element_type=F32)


def iota(shape, dim):
    return lax.broadcasted_iota(jnp.int32, shape, dim)


def entry_slots(row, var, carry_ref, owners):
    bound = row.shape[1]
    live = row >= 0
    owner = jnp.where(live, lax.shift_right_arithmetic(var, 6), -1)
    owned = iota((owners, bound), 0) == owner
    owned_f = owned.astype(F32)
    before = (iota((bound, bound), 0) < iota((bound, bound), 1)).astype(F32).astype(BF16)
    earlier = dot(owned_f.astype(BF16), before)
    rank = jnp.sum(jnp.where(owned, earlier + carry_ref[...], 0.0), axis=0, keepdims=True)
    carry_ref[...] += jnp.sum(owned_f, axis=1, keepdims=True)
    return jnp.where(live, owner * SLOT + rank.astype(jnp.int32), -1)


def placing(slot, slots):
    return (iota((slots, slot.shape[1]), 0) == slot).astype(F32).astype(BF16)


def picking(row, state):
    bound = row.shape[1]
    down = jnp.broadcast_to(row.astype(F32), (bound, bound)).T.astype(jnp.int32)
    lane = iota((bound, bound), 1)
    parts = [(lane + at == down).astype(F32) for at in range(0, state, bound)]
    return jnp.concatenate(parts, axis=1).astype(BF16)


def start_kernel(
    row_ref, var_ref, ginv_ref, rhs_ref, local_ref, out_ref, couple_ref,
    block_ref, right_ref, picked_ref, carry_ref, place_ref, solved_ref,
    block_sems, right_sems,
):
    areas, bound = row_ref.shape
    state = ginv_ref.shape[1]
    slots, snaps = local_ref.shape
    owners = slots // SLOT

    def block_copy(area):
        return pltpu.make_async_copy(ginv_ref.at[area], block_ref.at[area], block_sems.at[area])

    def right_copy(area):
        rows = pl.ds(area * state, state)
        return pltpu.make_async_copy(rhs_ref.at[rows], right_ref.at[rows], right_sems.at[area])

    for area in range(areas):
        block_copy(area).start()
        right_copy(area).start()
    carry_ref[...] = jnp.zeros_like(carry_ref)
    picks = []
    columns = []
    local_ids = []
    for area in range(areas):
        row = row_ref[area : area + 1, :]
        var = var_ref[area : area + 1, :]
        place_ref[:, area * bound : (area + 1) * bound] = placing(
            entry_slots(row, var, carry_ref, owners), slots
        )
        picks.append(picking(row, state))
        columns.append(placing(row, state))
        local_id = jnp.where(row >= 0, (var & (VAR_DEV - 1)) + 1, 0).astype(F32)
        local_ids.append(jnp.broadcast_to(local_id, (snaps, bound)).T.astype(BF16))
    local_ids = jnp.concatenate(local_ids, axis=0)
    for at in range(0, slots, PIECE):
        local_ref[at : at + PIECE, :] = dot(place_ref[at : at + PIECE, :], local_ids)
    lane = iota((owners, snaps), 1)
    ids = jnp.zeros((owners, snaps), F32)
    for k in range(SLOT):
        ids += jnp.where(lane == k, local_ref[pl.ds(k, owners, stride=SLOT), :], 0.0)
    out_ref[pl.ds(SLOT, owners, stride=WIDE), :] = ids
    for area in range(areas):
        block_copy(area).wait()
        right_copy(area).wait()
        for at in range(0, state, BUILD):
            part = dot(picks[area], block_ref[area, :, at : at + BUILD])
            picked_ref[:, at : at + BUILD] = part.astype(BF16)
        right = right_ref[area * state : (area + 1) * state, :].astype(BF16)
        both = dot(picked_ref[...], jnp.concatenate([right, columns[area]], axis=1))
        solved = both[:, :snaps]
        couple_ref[area] = both[:, snaps:].astype(BF16)
        solved_ref[area * bound : (area + 1) * bound, :] = jnp.concatenate(split3(solved), axis=1)
    for at in range(0, slots, PIECE):
        local_ref[at : at + PIECE, :] = join3(dot(place_ref[at : at + PIECE, :], solved_ref[...]), 0, snaps)
    for k in range(SLOT):
        at = pl.ds(k, owners, stride=SLOT)
        out_ref[pl.ds(k, owners, stride=WIDE), :] = local_ref[at, :]


def prepare_kernel(
    row_ref, var_ref, couple_ref, rhs_ref, ginv_ref,
    back_ref, mat_ref, term_ref, inner_ref, first_ref, cols_ref,
    right_ref, kept_ref, carry_ref, rows_ref, spread_ref, place_ref,
    block_ref, right_sems, out_sems, block_sem,
):
    areas, bound = row_ref.shape
    state = rhs_ref.shape[0] // areas
    slots, snaps = term_ref.shape

    def right_copy(area):
        rows = pl.ds(area * state, state)
        return pltpu.make_async_copy(rhs_ref.at[rows], right_ref.at[rows], right_sems.at[area])

    def out_copy(area):
        rows = pl.ds(area * state, state)
        return pltpu.make_async_copy(kept_ref.at[rows], inner_ref.at[rows], out_sems.at[area])

    block_copy = pltpu.make_async_copy(ginv_ref.at[0], block_ref, block_sem.at[0])
    for area in range(areas):
        right_copy(area).start()
        if area == 0:
            block_copy.start()
    carry_ref[...] = jnp.zeros_like(carry_ref)
    for area in range(areas):
        var = var_ref[area : area + 1, :]
        slot = entry_slots(row_ref[area : area + 1, :], var, carry_ref, slots // SLOT)
        entries = slice(area * bound, (area + 1) * bound)
        place_ref[:, entries] = placing(slot, slots)
        back_ref[entries, :] = picking(slot, slots)
    ones = jnp.ones((bound, snaps), BF16)
    for area in range(areas):
        entries = slice(area * bound, (area + 1) * bound)
        row = row_ref[area : area + 1, :]
        right_copy(area).wait()
        for at in range(0, state, BUILD):
            here = slice(area * state + at, area * state + at + BUILD)
            is_bound = dot(placing(row - at, BUILD), ones) > 0.0
            kept_ref[here, :] = jnp.where(is_bound, 0.0, right_ref[here, :]).astype(BF16)
        out_copy(area).start()
        right = right_ref[area * state : (area + 1) * state, :]
        at_rows = dot(picking(row, state), jnp.concatenate(split3(right), axis=1))
        rows_ref[entries, :] = at_rows.astype(BF16)
        for at in range(0, slots, PIECE):
            spread = dot(place_ref[at : at + PIECE, entries], couple_ref[area])
            spread_ref[at : at + PIECE, entries] = spread.astype(BF16)
    block_copy.wait()
    columns = placing(row_ref[0:1, :], state)
    columns = jnp.concatenate([kept_ref[:state, :], columns], axis=1)
    for at in range(0, state, PIECE):
        both = dot(block_ref[at : at + PIECE, :], columns)
        first_ref[at : at + PIECE, :] = both[:, :snaps]
        cols_ref[at : at + PIECE, :] = both[:, snaps:].astype(BF16)
    for at in range(0, slots, PIECE):
        here = slice(at, at + PIECE)
        term_ref[here, :] = join3(dot(place_ref[here, :], rows_ref[...]), 0, snaps)
        mat_ref[here, :] = dot(spread_ref[here, :], back_ref[...]).astype(BF16)
    for area in range(areas):
        out_copy(area).wait()


def first_owner_kernel(in_ref, ret_ref, member_ref, inverse_ref):
    sources = in_ref.shape[0] // WIDE
    snaps = in_ref.shape[1]
    ids = in_ref[pl.ds(SLOT, sources, stride=WIDE), :].astype(jnp.int32)
    lane = iota((sources, 128), 1) + 1
    parts = [(ids[:, k : k + 1] == lane).astype(F32) for k in range(SLOT)]
    for k in range(SLOT):
        member_ref[pl.ds(k, sources, stride=SLOT), :] = parts[k][:, :VAR_DEV]
    member = jnp.concatenate(parts, axis=0).astype(BF16)
    values = [in_ref[pl.ds(k, sources, stride=WIDE), :] for k in range(SLOT)]
    values = jnp.concatenate(values, axis=0)
    columns = jnp.concatenate(split3(values) + [jnp.ones(values.shape, BF16)], axis=1)
    sums = dot_t(member, columns)
    inverse = 1.0 / jnp.maximum(sums[:, 3 * snaps :], 1.0)
    inverse_ref[...] = inverse[:VAR_DEV]
    consensus = join3(sums, 0, snaps) * inverse
    back = join3(dot(member, jnp.concatenate(split3(consensus), axis=1)), 0, snaps)
    for k in range(SLOT):
        ret_ref[pl.ds(k, sources, stride=SLOT), :] = back[k * sources : (k + 1) * sources]


def states_kernel(
    row_ref, ginv_ref, inner_ref, first_ref, cols_ref, back_ref, blend_ref, states_ref,
    block_ref, right_ref, solved_ref, made_ref, made_cols_ref,
    block_sems, right_sems, out_sems, made_sems,
):
    areas, bound = row_ref.shape
    state = ginv_ref.shape[1]

    def rows_of(area):
        return pl.ds(area * state, state)

    def right_copy(area):
        rows = rows_of(area)
        return pltpu.make_async_copy(inner_ref.at[rows], right_ref.at[rows], right_sems.at[area])

    def block_copy(area):
        return pltpu.make_async_copy(ginv_ref.at[area], block_ref.at[area - 1], block_sems.at[area])

    def out_copy(piece):
        rows = pl.ds(piece * OUT, OUT)
        return pltpu.make_async_copy(solved_ref.at[rows], states_ref.at[rows], out_sems.at[piece])

    made_copy = pltpu.make_async_copy(first_ref, made_ref, made_sems.at[0])
    made_cols_copy = pltpu.make_async_copy(cols_ref, made_cols_ref, made_sems.at[1])
    made_copy.start()
    made_cols_copy.start()
    for area in range(1, areas):
        right_copy(area).start()
        block_copy(area).start()
    entry_rows = dot(back_ref[...], blend_ref[...]).astype(BF16)
    made_copy.wait()
    made_cols_copy.wait()
    for at in range(0, state, PIECE):
        here = slice(at, at + PIECE)
        solved_ref[here, :] = made_ref[here, :] + dot(made_cols_ref[here, :], entry_rows[:bound])
    for piece in range(state // OUT):
        out_copy(piece).start()
    for area in range(1, areas):
        row = row_ref[area : area + 1, :]
        rows = entry_rows[area * bound : (area + 1) * bound]
        right_copy(area).wait()
        pieces = []
        for at in range(0, state, BUILD):
            placed = dot(placing(row - at, BUILD), rows).astype(BF16)
            pieces.append(right_ref[area * state + at : area * state + at + BUILD, :] + placed)
        blended = jnp.concatenate(pieces, axis=0)
        block_copy(area).wait()
        for at in range(0, state, PIECE):
            solved = dot(block_ref[area - 1, at : at + PIECE, :], blended)
            solved_ref[area * state + at : area * state + at + PIECE, :] = solved
            if (at + PIECE) % OUT == 0:
                out_copy((area * state + at) // OUT).start()
    for piece in range(areas * state // OUT):
        out_copy(piece).wait()


def select(spec, a, b):
    return jnp.einsum(spec, a, b, precision=lax.Precision.HIGH, preferred_element_type=F32)


def shape(dims, dtype=F32):
    return jax.ShapeDtypeStruct(dims, dtype)


def on_device(ginv, rhs, bnd_row, bnd_var):
    areas, state, _ = ginv.shape
    snaps = rhs.shape[1]
    bound = bnd_row.shape[1]
    devices = lax.axis_size("area") * lax.axis_size("tie")
    slots = devices * SLOT
    entries = areas * bound

    anywhere = pl.BlockSpec(memory_space=pl.ANY)
    small = pl.BlockSpec((areas, bound), lambda: (0, 0))
    whole = pl.BlockSpec(memory_space=pltpu.VMEM)
    local, outgoing, couple = pl.pallas_call(
        start_kernel,
        in_specs=[small, small, anywhere, anywhere],
        out_specs=[whole, whole, whole],
        out_shape=[
            pltpu.VMEM((slots, snaps), F32),
            pltpu.VMEM((devices * WIDE, snaps), F32),
            shape((areas, bound, bound), BF16),
        ],
        scratch_shapes=[
            pltpu.VMEM((areas, state, state), BF16),
            pltpu.VMEM((areas * state, snaps), F32),
            pltpu.VMEM((bound, state), BF16),
            pltpu.VMEM((devices, bound), F32),
            pltpu.VMEM((slots, entries), BF16),
            pltpu.VMEM((entries, 3 * snaps), BF16),
            pltpu.SemaphoreType.DMA((areas,)),
            pltpu.SemaphoreType.DMA((areas,)),
        ],
        name="start",
    )(bnd_row, bnd_var, ginv, rhs)
    back, mat, term, inner, first, cols = pl.pallas_call(
        prepare_kernel,
        in_specs=[small, small, whole, anywhere, anywhere],
        out_specs=[whole, whole, whole, anywhere, whole, whole],
        out_shape=[
            pltpu.VMEM((entries, slots), BF16),
            pltpu.VMEM((slots, slots), BF16),
            pltpu.VMEM((slots, snaps), F32),
            shape((areas * state, snaps), BF16),
            shape((state, snaps)),
            shape((state, bound), BF16),
        ],
        scratch_shapes=[
            pltpu.VMEM((areas * state, snaps), F32),
            pltpu.VMEM((areas * state, snaps), BF16),
            pltpu.VMEM((devices, bound), F32),
            pltpu.VMEM((entries, 3 * snaps), BF16),
            pltpu.VMEM((slots, entries), BF16),
            pltpu.VMEM((slots, entries), BF16),
            pltpu.VMEM((state, state), BF16),
            pltpu.SemaphoreType.DMA((areas,)),
            pltpu.SemaphoreType.DMA((areas,)),
            pltpu.SemaphoreType.DMA((1,)),
        ],
        name="prepare",
    )(bnd_row, bnd_var, couple, rhs, ginv)

    def exchange(x, rows=SLOT, width=snaps):
        x = x.reshape(devices, rows, width)
        x = lax.all_to_all(x, ("area", "tie"), split_axis=0, concat_axis=0, tiled=True)
        return x.reshape(-1, snaps)

    base = local - dot(mat, term.astype(BF16))
    received, back, mat, base, term, inner, first, cols = lax.optimization_barrier(
        (exchange(outgoing, 1, WIDE * snaps), back, mat, base, term, inner, first, cols)
    )
    returning, member, inverse = pl.pallas_call(
        first_owner_kernel,
        in_specs=[whole],
        out_shape=[
            pltpu.VMEM((slots, snaps), F32),
            pltpu.VMEM((slots, VAR_DEV), F32),
            pltpu.VMEM((VAR_DEV, snaps), F32),
        ],
        name="first_owner",
    )(pltpu.with_memory_space_constraint(received, pltpu.VMEM))
    for iteration in range(ITERS):
        if iteration > 0:
            blend = (term + PENALTY * (agreed - dual)).astype(BF16)
            local = (base + dot(mat, blend)) + dual
            consensus = select("sv,sn->vn", member, exchange(local)) * inverse
            returning = select("sv,vn->sn", member, consensus)
        agreed = exchange(returning)
        dual = local - agreed
    states = pl.pallas_call(
        states_kernel,
        in_specs=[
            small,
            anywhere,
            anywhere,
            anywhere,
            anywhere,
            pl.BlockSpec((entries, slots), lambda: (0, 0)),
            pl.BlockSpec((slots, snaps), lambda: (0, 0)),
        ],
        out_specs=anywhere,
        out_shape=shape((areas * state, snaps)),
        scratch_shapes=[
            pltpu.VMEM((areas - 1, state, state), BF16),
            pltpu.VMEM((areas * state, snaps), BF16),
            pltpu.VMEM((areas * state, snaps), F32),
            pltpu.VMEM((state, snaps), F32),
            pltpu.VMEM((state, bound), BF16),
            pltpu.SemaphoreType.DMA((areas,)),
            pltpu.SemaphoreType.DMA((areas,)),
            pltpu.SemaphoreType.DMA((areas * state // OUT,)),
            pltpu.SemaphoreType.DMA((2,)),
        ],
        name="states",
    )(bnd_row, ginv, inner, first, cols, back, blend)
    dual = select("es,sn->en", back.astype(F32), dual)
    return states, consensus, dual


def solution(mesh):
    both = ("area", "tie")
    return jax.shard_map(
        on_device,
        mesh=mesh,
        in_specs=(P(both, None, None), P(both, None), P(both, None), P(both, None)),
        out_specs=(P(both, None), P(both, None), P(both, None)),
        check_vma=False,
    )
```
